256 devices in a mesh: group: 8 (over z), shard: 32 (over x, y, core).
Axes of the slice: x: 4, y: 4, z: 8, core: 2. Of those that a mesh axis runs over, the one named last changes fastest.
Arguments:
- queries: bfloat16 [1536, 1024], P(('group', 'shard')), may hold values from -12 to 12
- candidates: bfloat16 [1048576, 1024], P(('group', 'shard')), may hold values from -4 to 4
- targets: int32 [1536], replicated, may hold values from 0 to 1048575
Outputs:
- losses: float32 [1536], replicated
- mean_loss: float32 [], replicated
The draws below stay inside these ranges and needn't reach their ends.
All inputs are finite; a program needn't handle non-finite values.
Results may differ from the reference program's by a relative error of at most 0.0003.
Values may be sent and summed in bfloat16 or wider, within the bound.
A program may use at most 64 MiB of HBM per device.

```python
import jax
import jax.numpy as jnp
from jax import lax

D = 1024
CAND_DEV = 4096
QUERIES = 1536
CANDS = 1048576
N_GROUP = 8
N_SHARD = 32


def shared_queries(key):
    normal_key = jax.random.fold_in(key, 11)
    base = jnp.clip(jax.random.normal(normal_key, (QUERIES, D), jnp.float32), -6.0, 6.0)
    return base


def draw_queries(key, part):
    base = shared_queries(key)
    return base.astype(jnp.bfloat16)


def draw_candidates(key, part):
    cand_key = jax.random.fold_in(key, 21)
    size_key = jax.random.fold_in(key, 22)
    order_key = jax.random.fold_in(key, 31)
    offset_key = jax.random.fold_in(key, 32)
    height_key = jax.random.fold_in(key, 33)
    row_sizes = 0.5 * jnp.exp(jax.random.uniform(size_key, (CANDS, 1), jnp.float32, 0.0, 1.0) * jnp.log(8.0))
    rows = jnp.clip(jax.random.normal(cand_key, (CANDS, D), jnp.float32), -6.0, 6.0)
    rows = rows * row_sizes * D ** (-0.5)
    base = shared_queries(key)
    plant_norms = 0.5 * jnp.exp(jax.random.uniform(height_key, (QUERIES,), jnp.float32, 0.0, 1.0) * jnp.log(8.0))
    heights = plant_norms * D ** (-0.5)
    strong = jnp.arange(QUERIES, dtype=jnp.int32) < 8
    heights = jnp.where(strong, jnp.float32(min(4.0, 300.0 / D)), heights)
    aligned = jnp.where(base >= 0.0, heights[:, None], -heights[:, None])
    stride = CANDS // QUERIES
    order = jax.random.permutation(order_key, QUERIES).astype(jnp.int32)
    offsets = jax.random.randint(offset_key, (QUERIES,), 0, stride, jnp.int32)
    places = order * stride + offsets
    rows = rows.at[places].set(aligned)
    return rows.astype(jnp.bfloat16)


def plant(values, own_key, least, top_value):
    index_at = [jax.random.randint(jax.random.fold_in(own_key, axis), (), 0, length) for axis, length in enumerate(values.shape)]
    widest = values.shape.index(max(values.shape))
    beside = index_at[:widest] + [(index_at[widest] + 1) % values.shape[widest]] + index_at[widest + 1:]
    return values.at[tuple(index_at)].set(least).at[tuple(beside)].set(top_value)


def setup_inputs(seed: int = 0) -> dict:
    arg_keys = jax.random.split(jax.random.key(seed), 4)
    queries = draw_queries(jax.random.fold_in(arg_keys[3], 71), 0)
    candidates = draw_candidates(jax.random.fold_in(arg_keys[3], 71), 0)
    targets = plant(jax.random.randint(arg_keys[2], (QUERIES,), 0, CANDS), jax.random.fold_in(arg_keys[2], 1), 0, CANDS - 1).astype(jnp.int32)
    return dict(queries=queries, candidates=candidates, targets=targets)


def reference(queries, candidates, targets):
    blocks = candidates.reshape(N_GROUP * N_SHARD, CAND_DEV, D)

    def step(carry, block):
        top, total = carry
        scores = jnp.dot(queries, block.T, preferred_element_type=jnp.float32)
        block_top = jnp.max(scores, axis=1)
        new_top = jnp.maximum(top, block_top)
        total = total * jnp.exp(top - new_top) + jnp.sum(jnp.exp(scores - new_top[:, None]), axis=1)
        return (new_top, total), None

    start = (jnp.full((QUERIES,), -jnp.inf, jnp.float32), jnp.zeros((QUERIES,), jnp.float32))
    (top, total), unused = lax.scan(step, start, blocks)
    chosen = jnp.take(candidates, targets.astype(jnp.int32), axis=0)
    picked = jnp.sum(queries.astype(jnp.float32) * chosen.astype(jnp.float32), axis=1)
    losses = top + jnp.log(total) - picked
    return losses, jnp.mean(losses)
```

```python
import functools

import jax
import jax.numpy as jnp
from jax import lax
from jax.experimental import pallas as pl
from jax.experimental.pallas import tpu as pltpu
from jax.sharding import PartitionSpec as P

F32 = jnp.float32
BF16 = jnp.bfloat16
MESH = pl.DeviceIdType.MESH
LOW = -3.0e38
PER = 6
BLOCK = 48
UNIT = 192
OWN = {0: 0, 1: 2, 3: 3, 2: 6}
OTHER = {0: 1, 1: 4, 3: 5, 2: 7}
NEAR_FIRST = (1, 3, 2)


def place():
    z = lax.axis_index("group")
    s = lax.axis_index("shard")
    x, y, c = s // 8, (s // 2) % 4, s % 2
    u = y * (1 - c) + x * c
    v = x * (1 - c) + y * c
    return z, u, v, c


def at(z, u, v, c):
    x = v * (1 - c) + u * c
    y = u * (1 - c) + v * c
    return (z, (x * 4 + y) * 2 + c)


def rows_of(slot, v):
    return pl.ds(pl.multiple_of(slot * UNIT + v * BLOCK, 16), BLOCK)


def meet(others):
    barrier = pltpu.get_barrier_semaphore()
    for other in others:
        pl.semaphore_signal(barrier, inc=1, device_id=other, device_id_type=MESH)
    pl.semaphore_wait(barrier, len(others))


def gather_kernel(q_ref, all_ref, first, send1, recv1, send2, recv2, send3, recv3, sendp, recvp):
    z, u, v, c = place()
    partner = (z, at(z, u, v, c)[1] + 1 - 2 * c)
    column = [at((z + d) % 8, u, v, c) for d in range(1, 8)]
    along_v = {d: at(z, u, (v + d) % 4, c) for d in NEAR_FIRST}
    along_u = {d: at(z, (u + d) % 4, v, c) for d in NEAR_FIRST}
    meet(column + list(along_v.values()) + list(along_u.values()) + [partner])

    def copy(src, dst, send, recv, to):
        return pltpu.make_async_remote_copy(
            src_ref=src, dst_ref=dst, send_sem=send, recv_sem=recv, device_id=to, device_id_type=MESH
        )

    first[z] = q_ref[...]
    sent = []
    for d in (4, 3, 5, 2, 6, 1, 7):
        one = copy(q_ref, first.at[z], send1.at[d], recv1.at[d], column[d - 1])
        one.start()
        sent.append(one)
    for d in (1, 7, 2, 6, 3, 5, 4):
        here = first.at[(z + 8 - d) % 8]
        copy(here, here, send1.at[d], recv1.at[d], column[d - 1]).wait_recv()
    block = jnp.concatenate([first[k].astype(F32) for k in range(8)], axis=0)
    all_ref[rows_of(0, v), :] = block.astype(BF16)

    def pass_on(d):
        src = (v + 4 - d) % 4
        held = all_ref.at[rows_of(0, src)]
        to = [(held, OTHER[0], sendp.at[0, d], recvp.at[0, d], partner)]
        for e in NEAR_FIRST:
            to.append((held, OWN[(4 - e) % 4], send3.at[e, d], recv3.at[e, d], along_u[e]))
        for held, slot, send, recv, device in to:
            one = copy(held, all_ref.at[rows_of(slot, src)], send, recv, device)
            one.start()
            sent.append(one)

    own = all_ref.at[rows_of(0, v)]
    for d in NEAR_FIRST:
        one = copy(own, own, send2.at[d], recv2.at[d], along_v[d])
        one.start()
        sent.append(one)
    pass_on(0)
    for d in NEAR_FIRST:
        here = all_ref.at[rows_of(0, (v + 4 - d) % 4)]
        copy(here, here, send2.at[d], recv2.at[d], along_v[d]).wait_recv()
        pass_on(d)
    for d in (0, 1, 3, 2):
        for e in NEAR_FIRST:
            far = (4 - e) % 4
            src = (v + 4 - d) % 4
            here = all_ref.at[rows_of(OWN[far], src)]
            copy(here, here, send3.at[e, d], recv3.at[e, d], along_u[e]).wait_recv()
            one = copy(here, all_ref.at[rows_of(OTHER[far], src)], sendp.at[far, d], recvp.at[far, d], partner)
            one.start()
            sent.append(one)
    for far in (0, 1, 3, 2):
        for d in range(4):
            here = all_ref.at[rows_of(OTHER[far], (u + 4 - d) % 4)]
            copy(here, here, sendp.at[far, d], recvp.at[far, d], partner).wait_recv()
    for one in sent:
        one.wait_send()


def gather(queries):
    dma = pltpu.SemaphoreType.DMA
    return pl.pallas_call(
        gather_kernel,
        out_shape=jax.ShapeDtypeStruct((8 * UNIT, queries.shape[1]), BF16),
        in_specs=[pl.BlockSpec(memory_space=pltpu.VMEM)],
        out_specs=pl.BlockSpec(memory_space=pltpu.VMEM),
        scratch_shapes=[pltpu.VMEM((8, PER, queries.shape[1]), BF16)]
        + [dma((8,)), dma((8,)), dma((4,)), dma((4,)), dma((4, 4)), dma((4, 4)), dma((4, 4)), dma((4, 4))],
        compiler_params=pltpu.CompilerParams(collective_id=1, has_side_effects=True),
        name="gather_queries",
    )(queries)


def score_kernel(rows, cols, q_ref, c_hbm, t_ref, o_ref, c_buf, s0, s1, sem):
    count = c_buf.shape[0]
    blocks = count // rows
    chunk = 1024
    loads = [
        pltpu.make_async_copy(c_hbm.at[pl.ds(i * chunk, chunk)], c_buf.at[pl.ds(i * chunk, chunk)], sem.at[i])
        for i in range(count // chunk)
    ]
    for load in loads:
        load.start()
    for load in loads:
        load.wait()
    groups = rows // 8
    z, u, v, c = place()

    def scored(q, k):
        part = c_buf[pl.ds(pl.multiple_of(k * rows, rows), rows), :]
        return lax.dot_general(part, q, (((1,), (1,)), ((), ())), preferred_element_type=F32)

    def peak(scores, top):
        return jnp.maximum(top, jnp.max(scores.reshape(groups, 8, cols), axis=0))

    results = []
    for batch in range(q_ref.shape[0] // cols):
        q_rows = pl.ds(batch * cols, cols)
        wanted = jnp.broadcast_to(t_ref[:, batch * cols : (batch + 1) * cols], (8, cols))
        wanted = wanted - lax.broadcasted_iota(jnp.int32, (8, cols), 0)

        def take(held, k, old, new, total, picked, wanted=wanted):
            total = total * jnp.exp(old - new)
            for g in range(groups):
                value = held[g * 8 : (g + 1) * 8, :]
                total = total + jnp.exp(value - new)
                picked = jnp.where(wanted == k * rows + g * 8, value, picked)
            return total, picked

        def step(j, carry, q_rows=q_rows, take=take):
            old, new, total, picked = carry
            scores = scored(q_ref[q_rows, :], 2 * j + 1)
            s1[...] = scores
            newer = peak(scores, new)
            total, picked = take(s0, 2 * j, old, new, total, picked)
            scores = scored(q_ref[q_rows, :], 2 * j + 2)
            s0[...] = scores
            newest = peak(scores, newer)
            total, picked = take(s1, 2 * j + 1, new, newer, total, picked)
            return newer, newest, total, picked

        old = jnp.full((8, cols), LOW, F32)
        zero = jnp.zeros((8, cols), F32)
        scores = scored(q_ref[q_rows, :], 0)
        s0[...] = scores
        carry = (old, peak(scores, old), zero, zero)
        old, new, total, picked = lax.fori_loop(0, blocks // 2 - 1, step, carry)
        scores = scored(q_ref[q_rows, :], blocks - 1)
        s1[...] = scores
        newer = peak(scores, new)
        total, picked = take(s0, blocks - 2, old, new, total, picked)
        total, picked = take(s1, blocks - 1, new, newer, total, picked)
        top = jnp.max(newer, axis=0, keepdims=True)
        total = jnp.sum(total * jnp.exp(newer - top), axis=0, keepdims=True)
        results.append((top, total, jnp.sum(picked, axis=0, keepdims=True)))
    lines = [jnp.concatenate(parts, axis=1) for parts in zip(*results)]
    for far in range(4):
        for slot, unit in ((OWN[far], c * 4 + (u + far) % 4), (OTHER[far], (1 - c) * 4 + (v + far) % 4)):
            parts = []
            for line in lines:
                parts.append(line[:, slot * UNIT : slot * UNIT + 128])
                parts.append(line[:, slot * UNIT + 64 : slot * UNIT + 192])
            o_ref[unit] = jnp.concatenate(parts + [jnp.zeros((2, 128), F32)], axis=0)


def score(queries, candidates, targets, rows=512, cols=512):
    count, width = candidates.shape
    return pl.pallas_call(
        functools.partial(score_kernel, rows, cols),
        out_shape=jax.ShapeDtypeStruct((8, 8, 128), F32),
        in_specs=[
            pl.BlockSpec(memory_space=pltpu.VMEM),
            pl.BlockSpec(memory_space=pl.ANY),
            pl.BlockSpec(memory_space=pltpu.VMEM),
        ],
        out_specs=pl.BlockSpec(memory_space=pltpu.VMEM),
        scratch_shapes=[
            pltpu.VMEM((count, width), BF16),
            pltpu.VMEM((rows, cols), F32),
            pltpu.VMEM((rows, cols), F32),
            pltpu.SemaphoreType.DMA((count // 1024,)),
        ],
        compiler_params=pltpu.CompilerParams(vmem_limit_bytes=50 << 20),
        name="score_queries",
    )(queries, candidates, targets)


def combined(tiles):
    tops = [tile[0:2] for tile in tiles]
    top = functools.reduce(jnp.maximum, tops)
    total = sum(tile[2:4] * jnp.exp(one - top) for tile, one in zip(tiles, tops))
    picked = sum(tile[4:6] for tile in tiles)
    return jnp.concatenate([top, total, picked, jnp.zeros((2, 128), F32)], axis=0)


def reduce_kernel(r_ref, o_ref, from_core, at_x, from_x, at_y, from_y, at_z, from_z, mine, sends, recvs):
    z = lax.axis_index("group")
    s = lax.axis_index("shard")
    x, y, c = s // 8, (s // 2) % 4, s % 2

    def device(z, x, y, c):
        return (z, (x * 4 + y) * 2 + c)

    partner = device(z, x, y, 1 - c)
    xs = [device(z, (x + d) % 4, y, c) for d in range(1, 4)]
    crossed = [device(z, (x + d) % 4, y, 1 - c) for d in range(1, 4)]
    ys = [device(z, x, (y + d) % 4, c) for d in range(1, 4)]
    zs = [device((z + d) % 8, x, y, c) for d in range(1, 8)]
    meet([partner] + xs + crossed + ys + zs)

    def copy(k, src, dst, to):
        return pltpu.make_async_remote_copy(
            src_ref=src, dst_ref=dst, send_sem=sends.at[k], recv_sem=recvs.at[k], device_id=to, device_id_type=MESH
        )

    half = pl.ds((1 - c) * 4, 4)
    one = copy(0, r_ref.at[half], from_core, partner)
    one.start()
    sent = [one]
    one.wait_recv()
    for k in range(4):
        at_x[k] = combined([r_ref[c * 4 + k], from_core[k]])
    for d in range(1, 4):
        one = copy(d, at_x.at[(x + d) % 4], from_x.at[d], xs[d - 1])
        one.start()
        sent.append(one)
    for one in sent[1:4]:
        one.wait_recv()
    at_y[...] = combined([at_x[x]] + [from_x[d] for d in range(1, 4)])
    for d in range(1, 4):
        one = copy(3 + d, at_y, from_y.at[d], ys[d - 1])
        one.start()
        sent.append(one)
    for one in sent[4:7]:
        one.wait_recv()
    at_z[...] = combined([at_y[...]] + [from_y[d] for d in range(1, 4)])
    for d in (4, 3, 5, 2, 6, 1, 7):
        one = copy(6 + d, at_z, from_z.at[d], zs[d - 1])
        one.start()
        sent.append(one)
    for one in sent[7:14]:
        one.wait_recv()
    whole = combined([at_z[...]] + [from_z[d] for d in range(1, 8)])
    loss = whole[0:2] + jnp.log(whole[2:4]) - whole[4:6]
    mine[...] = jnp.concatenate([loss, jnp.zeros((6, 128), F32)], axis=0)
    unit = c * 4 + x
    o_ref[unit] = mine[...]
    for d in range(7):
        one = copy(14 + d, mine, o_ref.at[unit], ([partner] + xs + crossed)[d])
        one.start()
        sent.append(one)
    for d in range(7):
        other = c * 4 if 1 <= d < 4 else (1 - c) * 4
        here = o_ref.at[other + (x + 4 - (0, 1, 2, 3, 1, 2, 3)[d]) % 4]
        copy(14 + d, mine, here, partner).wait_recv()
    for one in sent:
        one.wait_send()


def reduced(partial):
    tile = (8, 128)
    dma = pltpu.SemaphoreType.DMA
    return pl.pallas_call(
        reduce_kernel,
        out_shape=jax.ShapeDtypeStruct((8, *tile), F32),
        in_specs=[pl.BlockSpec(memory_space=pltpu.VMEM)],
        out_specs=pl.BlockSpec(memory_space=pltpu.VMEM),
        scratch_shapes=[
            pltpu.VMEM((4, *tile), F32),
            pltpu.VMEM((4, *tile), F32),
            pltpu.VMEM((4, *tile), F32),
            pltpu.VMEM(tile, F32),
            pltpu.VMEM((4, *tile), F32),
            pltpu.VMEM(tile, F32),
            pltpu.VMEM((8, *tile), F32),
            pltpu.VMEM(tile, F32),
            dma((21,)),
            dma((21,)),
        ],
        compiler_params=pltpu.CompilerParams(collective_id=2, has_side_effects=True),
        name="reduce_losses",
    )(partial)


def in_place_order(targets):
    t = targets.reshape(8, 4, 4, 2, PER)
    low = t[:, :, :, 0].transpose(2, 1, 0, 3).reshape(4, UNIT)
    high = t[:, :, :, 1].transpose(1, 2, 0, 3).reshape(4, UNIT)
    return jnp.stack([low, high])


def in_query_order(units):
    low = units[:4].reshape(4, 4, 8, PER).transpose(2, 1, 0, 3)
    high = units[4:].reshape(4, 4, 8, PER).transpose(2, 0, 1, 3)
    return jnp.stack([low, high], axis=3).reshape(-1)


def on_device(queries, candidates, targets):
    z, u, v, c = place()
    owner = z * 32 + lax.axis_index("shard")
    t = in_place_order(targets - owner * candidates.shape[0])
    slots = [None] * 8
    for far in range(4):
        slots[OWN[far]] = t[c, (u + far) % 4]
        slots[OTHER[far]] = t[1 - c, (v + far) % 4]
    every = gather(queries)
    partial = score(every, candidates, jnp.concatenate(slots)[None])
    out = reduced(partial)
    units = jnp.concatenate([out[:, 0], out[:, 1, 64:]], axis=1)
    losses = in_query_order(units)
    return losses, jnp.mean(losses)


def solution(mesh):
    whole = P(("group", "shard"), None)
    return jax.shard_map(
        on_device, mesh=mesh, in_specs=(whole, whole, P()), out_specs=(P(), P()), check_vma=False
    )
```

```python
import functools

import jax
import jax.numpy as jnp
from jax import lax
from jax.experimental import pallas as pl
from jax.experimental.pallas import tpu as pltpu
from jax.sharding import PartitionSpec as P

F32 = jnp.float32
BF16 = jnp.bfloat16
MESH = pl.DeviceIdType.MESH
LOW = -3.0e38
PER = 6
BLOCK = 48
UNIT = 192
OWN = {0: 0, 1: 2, 3: 3, 2: 6}
OTHER = {0: 1, 1: 4, 3: 5, 2: 7}
NEAR_FIRST = (1, 3, 2)
BATCHES = ((0, 256), (256, 512), (768, 512), (1280, 256))


def place():
    z = lax.axis_index("group")
    s = lax.axis_index("shard")
    x, y, c = s // 8, (s // 2) % 4, s % 2
    u = y * (1 - c) + x * c
    v = x * (1 - c) + y * c
    return z, u, v, c


def at(z, u, v, c):
    x = v * (1 - c) + u * c
    y = u * (1 - c) + v * c
    return (z, (x * 4 + y) * 2 + c)


def rows_of(slot, v):
    return pl.ds(pl.multiple_of(slot * UNIT + v * BLOCK, 16), BLOCK)


def meet(others):
    barrier = pltpu.get_barrier_semaphore()
    for other in others:
        pl.semaphore_signal(barrier, inc=1, device_id=other, device_id_type=MESH)
    pl.semaphore_wait(barrier, len(others))


def scored_batch(c_buf, q_ref, t_ref, first, cols, s0, s1):
    rows = s0.shape[0]
    blocks = c_buf.shape[0] // rows
    groups = rows // 8
    q_rows = pl.ds(first, cols)
    wanted = jnp.broadcast_to(t_ref[:, first : first + cols], (8, cols))
    wanted = wanted - lax.broadcasted_iota(jnp.int32, (8, cols), 0)

    def scored(k, held):
        part = c_buf[pl.ds(pl.multiple_of(k * rows, rows), rows), :]
        scores = lax.dot_general(part, q_ref[q_rows, :], (((1,), (1,)), ((), ())), preferred_element_type=F32)
        held[...] = scores
        return scores

    def peak(scores, top):
        return jnp.maximum(top, jnp.max(scores.reshape(groups, 8, cols), axis=0))

    def take(held, k, old, new, total, picked):
        total = total * jnp.exp(old - new)
        for g in range(groups):
            value = held[g * 8 : (g + 1) * 8, :]
            total = total + jnp.exp(value - new)
            picked = jnp.where(wanted == k * rows + g * 8, value, picked)
        return total, picked

    def step(j, carry):
        old, new, total, picked = carry
        newer = peak(scored(2 * j + 1, s1), new)
        total, picked = take(s0, 2 * j, old, new, total, picked)
        newest = peak(scored(2 * j + 2, s0), newer)
        total, picked = take(s1, 2 * j + 1, new, newer, total, picked)
        return newer, newest, total, picked

    old = jnp.full((8, cols), LOW, F32)
    zero = jnp.zeros((8, cols), F32)
    carry = (old, peak(scored(0, s0), old), zero, zero)
    old, new, total, picked = lax.fori_loop(0, blocks // 2 - 1, step, carry)
    newer = peak(scored(blocks - 1, s1), new)
    total, picked = take(s0, blocks - 2, old, new, total, picked)
    total, picked = take(s1, blocks - 1, new, newer, total, picked)
    top = jnp.max(newer, axis=0, keepdims=True)
    total = jnp.sum(total * jnp.exp(newer - top), axis=0, keepdims=True)
    return top, total, jnp.sum(picked, axis=0, keepdims=True)


def loss_kernel(
    q_ref, c_hbm, t_ref, o_ref,
    c_buf, all_ref, first, narrow0, narrow1, wide0, wide1,
    partial, from_core, at_x, from_x, at_y, from_y, at_z, from_z, mine,
    loaded, send1, recv1, send2, recv2, send3, recv3, sendp, recvp, sends, recvs,
):
    z, u, v, c = place()
    x = v * (1 - c) + u * c
    y = u * (1 - c) + v * c

    def device(z, x, y, c):
        return (z, (x * 4 + y) * 2 + c)

    chunk = c_buf.shape[0] // loaded.shape[0]
    loads = [
        pltpu.make_async_copy(c_hbm.at[pl.ds(i * chunk, chunk)], c_buf.at[pl.ds(i * chunk, chunk)], loaded.at[i])
        for i in range(loaded.shape[0])
    ]
    for load in loads:
        load.start()
    partner = device(z, x, y, 1 - c)
    column = [device((z + d) % 8, x, y, c) for d in range(1, 8)]
    xs = [device(z, (x + d) % 4, y, c) for d in range(1, 4)]
    ys = [device(z, x, (y + d) % 4, c) for d in range(1, 4)]
    crossed = [device(z, (x + d) % 4, y, 1 - c) for d in range(1, 4)]
    along_v = {d: at(z, u, (v + d) % 4, c) for d in NEAR_FIRST}
    along_u = {d: at(z, (u + d) % 4, v, c) for d in NEAR_FIRST}
    meet(column + xs + ys + crossed + [partner])
    sent = []

    def copy(src, dst, send, recv, to):
        return pltpu.make_async_remote_copy(
            src_ref=src, dst_ref=dst, send_sem=send, recv_sem=recv, device_id=to, device_id_type=MESH
        )

    def start(*args):
        one = copy(*args)
        one.start()
        sent.append(one)

    first[z] = q_ref[...]
    for d in (4, 3, 5, 2, 6, 1, 7):
        start(q_ref, first.at[z], send1.at[d], recv1.at[d], column[d - 1])
    for d in (1, 7, 2, 6, 3, 5, 4):
        here = first.at[(z + 8 - d) % 8]
        copy(here, here, send1.at[d], recv1.at[d], column[d - 1]).wait_recv()
    block = jnp.concatenate([first[k].astype(F32) for k in range(8)], axis=0)
    all_ref[rows_of(0, v), :] = block.astype(BF16)

    def to_partner(far, d):
        held = all_ref.at[rows_of(OWN[far], (v + 4 - d) % 4)]
        there = all_ref.at[rows_of(OTHER[far], (v + 4 - d) % 4)]
        start(held, there, sendp.at[far, d], recvp.at[far, d], partner)

    def along(e, d):
        held = all_ref.at[rows_of(0, (v + 4 - d) % 4)]
        there = all_ref.at[rows_of(OWN[(4 - e) % 4], (v + 4 - d) % 4)]
        start(held, there, send3.at[e, d], recv3.at[e, d], along_u[e])

    def arrived_along(e, d):
        here = all_ref.at[rows_of(OWN[(4 - e) % 4], (v + 4 - d) % 4)]
        copy(here, here, send3.at[e, d], recv3.at[e, d], along_u[e]).wait_recv()

    def from_partner(far):
        for d in range(4):
            here = all_ref.at[rows_of(OTHER[far], (u + 4 - d) % 4)]
            copy(here, here, sendp.at[far, d], recvp.at[far, d], partner).wait_recv()

    own = all_ref.at[rows_of(0, v)]
    for d in NEAR_FIRST:
        start(own, own, send2.at[d], recv2.at[d], along_v[d])
    to_partner(0, 0)
    along(1, 0)
    along(3, 0)
    for d in NEAR_FIRST:
        here = all_ref.at[rows_of(0, (v + 4 - d) % 4)]
        copy(here, here, send2.at[d], recv2.at[d], along_v[d]).wait_recv()
        to_partner(0, d)
        along(1, d)
        along(3, d)
    for d in (0, 1, 3, 2):
        along(2, d)
    for load in loads:
        load.wait()
    from_partner(0)

    results = []

    def run(k):
        begin, cols = BATCHES[k]
        held = (narrow0, narrow1) if cols == narrow0.shape[1] else (wide0, wide1)
        results.append(scored_batch(c_buf, all_ref, t_ref, begin, cols, *held))

    run(0)
    for d in (0, 1, 3, 2):
        for e in (1, 3):
            arrived_along(e, d)
            to_partner((4 - e) % 4, d)
    run(1)
    for d in (0, 1, 3, 2):
        arrived_along(2, d)
        to_partner(2, d)
    from_partner(1)
    from_partner(3)
    run(2)
    from_partner(2)
    run(3)

    lines = [jnp.concatenate(parts, axis=1) for parts in zip(*results)]
    for far in range(4):
        for slot, unit in ((OWN[far], c * 4 + (u + far) % 4), (OTHER[far], (1 - c) * 4 + (v + far) % 4)):
            parts = []
            for line in lines:
                parts.append(line[:, slot * UNIT : slot * UNIT + 128])
                parts.append(line[:, slot * UNIT + 64 : slot * UNIT + 192])
            partial[unit] = jnp.concatenate(parts + [jnp.zeros((2, 128), F32)], axis=0)

    def pass_on(k, src, dst, to):
        start(src, dst, sends.at[k], recvs.at[k], to)

    def wait(k, here):
        copy(here, here, sends.at[k], recvs.at[k], partner).wait_recv()

    pass_on(0, partial.at[pl.ds((1 - c) * 4, 4)], from_core, partner)
    wait(0, from_core)
    for k in range(4):
        at_x[k] = combined([partial[c * 4 + k], from_core[k]])
    for d in range(1, 4):
        pass_on(d, at_x.at[(x + d) % 4], from_x.at[d], xs[d - 1])
    for d in range(1, 4):
        wait(d, from_x.at[d])
    at_y[...] = combined([at_x[x]] + [from_x[d] for d in range(1, 4)])
    for d in range(1, 4):
        pass_on(3 + d, at_y, from_y.at[d], ys[d - 1])
    for d in range(1, 4):
        wait(3 + d, from_y.at[d])
    at_z[...] = combined([at_y[...]] + [from_y[d] for d in range(1, 4)])
    for d in (4, 3, 5, 2, 6, 1, 7):
        pass_on(6 + d, at_z, from_z.at[d], column[d - 1])
    for d in range(1, 8):
        wait(6 + d, from_z.at[d])
    whole = combined([at_z[...]] + [from_z[d] for d in range(1, 8)])
    loss = whole[0:2] + jnp.log(whole[2:4]) - whole[4:6]
    mine[...] = jnp.concatenate([loss, jnp.zeros((6, 128), F32)], axis=0)
    unit = c * 4 + x
    o_ref[unit] = mine[...]
    for d in range(7):
        pass_on(14 + d, mine, o_ref.at[unit], ([partner] + xs + crossed)[d])
    for d in range(7):
        colour = c * 4 if 1 <= d < 4 else (1 - c) * 4
        wait(14 + d, o_ref.at[colour + (x + 4 - (0, 1, 2, 3, 1, 2, 3)[d]) % 4])
    for one in sent:
        one.wait_send()


def all_losses(queries, candidates, targets):
    count, width = candidates.shape
    tile = (8, 128)
    dma = pltpu.SemaphoreType.DMA
    return pl.pallas_call(
        loss_kernel,
        out_shape=jax.ShapeDtypeStruct((8, *tile), F32),
        in_specs=[
            pl.BlockSpec(memory_space=pltpu.VMEM),
            pl.BlockSpec(memory_space=pl.ANY),
            pl.BlockSpec(memory_space=pltpu.VMEM),
        ],
        out_specs=pl.BlockSpec(memory_space=pltpu.VMEM),
        scratch_shapes=[
            pltpu.VMEM((count, width), BF16),
            pltpu.VMEM((8 * UNIT, width), BF16),
            pltpu.VMEM((8, PER, width), BF16),
            pltpu.VMEM((1024, 256), F32),
            pltpu.VMEM((1024, 256), F32),
            pltpu.VMEM((512, 512), F32),
            pltpu.VMEM((512, 512), F32),
            pltpu.VMEM((8, *tile), F32),
            pltpu.VMEM((4, *tile), F32),
            pltpu.VMEM((4, *tile), F32),
            pltpu.VMEM((4, *tile), F32),
            pltpu.VMEM(tile, F32),
            pltpu.VMEM((4, *tile), F32),
            pltpu.VMEM(tile, F32),
            pltpu.VMEM((8, *tile), F32),
            pltpu.VMEM(tile, F32),
        ]
        + [dma((4,)), dma((8,)), dma((8,)), dma((4,)), dma((4,)), dma((4, 4)), dma((4, 4)), dma((4, 4)), dma((4, 4))]
        + [dma((21,)), dma((21,))],
        compiler_params=pltpu.CompilerParams(
            collective_id=1, has_side_effects=True, vmem_limit_bytes=50 << 20
        ),
        name="ranking_losses",
    )(queries, candidates, targets)


def combined(tiles):
    tops = [tile[0:2] for tile in tiles]
    top = functools.reduce(jnp.maximum, tops)
    total = sum(tile[2:4] * jnp.exp(one - top) for tile, one in zip(tiles, tops))
    picked = sum(tile[4:6] for tile in tiles)
    return jnp.concatenate([top, total, picked, jnp.zeros((2, 128), F32)], axis=0)


def in_place_order(targets):
    t = targets.reshape(8, 4, 4, 2, PER)
    low = t[:, :, :, 0].transpose(2, 1, 0, 3).reshape(4, UNIT)
    high = t[:, :, :, 1].transpose(1, 2, 0, 3).reshape(4, UNIT)
    return jnp.stack([low, high])


def in_query_order(units):
    low = units[:4].reshape(4, 4, 8, PER).transpose(2, 1, 0, 3)
    high = units[4:].reshape(4, 4, 8, PER).transpose(2, 0, 1, 3)
    return jnp.stack([low, high], axis=3).reshape(-1)


def on_device(queries, candidates, targets):
    z, u, v, c = place()
    owner = z * 32 + lax.axis_index("shard")
    t = in_place_order(targets - owner * candidates.shape[0])
    slots = [None] * 8
    for far in range(4):
        slots[OWN[far]] = t[c, (u + far) % 4]
        slots[OTHER[far]] = t[1 - c, (v + far) % 4]
    out = all_losses(queries, candidates, jnp.concatenate(slots)[None])
    units = jnp.concatenate([out[:, 0], out[:, 1, 64:]], axis=1)
    losses = in_query_order(units)
    return losses, jnp.mean(losses)


def solution(mesh):
    whole = P(("group", "shard"), None)
    return jax.shard_map(
        on_device, mesh=mesh, in_specs=(whole, whole, P()), out_specs=(P(), P()), check_vma=False
    )
```

```python
import functools

import jax
import jax.numpy as jnp
from jax import lax
from jax.experimental import pallas as pl
from jax.experimental.pallas import tpu as pltpu
from jax.sharding import PartitionSpec as P

F32 = jnp.float32
BF16 = jnp.bfloat16
MESH = pl.DeviceIdType.MESH
LOW = -3.0e38
PER = 6
BLOCK = 48
UNIT = 192
OWN = {0: 0, 1: 2, 3: 3, 2: 6}
OTHER = {0: 1, 1: 4, 3: 5, 2: 7}
NEAR_FIRST = (1, 3, 2)
RELAYED_BY = (1, 3, 1, 3)
BATCHES = ((0, 256), (256, 512), (768, 512), (1280, 256))


def place():
    z = lax.axis_index("group")
    s = lax.axis_index("shard")
    x, y, c = s // 8, (s // 2) % 4, s % 2
    u = y * (1 - c) + x * c
    v = x * (1 - c) + y * c
    return z, u, v, c


def at(z, u, v, c):
    x = v * (1 - c) + u * c
    y = u * (1 - c) + v * c
    return (z, (x * 4 + y) * 2 + c)


def rows_of(slot, v):
    return pl.ds(pl.multiple_of(slot * UNIT + v * BLOCK, 16), BLOCK)


def meet(others):
    barrier = pltpu.get_barrier_semaphore()
    for other in others:
        pl.semaphore_signal(barrier, inc=1, device_id=other, device_id_type=MESH)
    pl.semaphore_wait(barrier, len(others))


def flat_place(l, colour, u):
    v = (l * 1366) >> 16
    l = l - v * BLOCK
    z = (l * 10923) >> 16
    r = l - z * PER
    chip = v * (4 - 3 * colour) + u * (1 + 3 * colour)
    return z * UNIT + chip * 2 * PER + colour * PER + r


def exact_parts(a):
    high = a.astype(BF16)
    rest = a - high.astype(F32)
    middle = rest.astype(BF16)
    return high, middle, (rest - middle.astype(F32)).astype(BF16)


def own_targets(targets, owner, rows, slots):
    local = targets - owner * rows
    local = jnp.where((local >= 0) & (local < rows), local, rows)
    pad = jnp.zeros((4, 128), jnp.int32)
    both = jnp.concatenate([local >> 6, pad, local & 63, pad], axis=0).astype(F32).astype(BF16)
    lines = []
    for colour, u in slots:
        flat = flat_place(lax.broadcasted_iota(jnp.int32, (1, UNIT), 1), colour, u)
        lane = lax.broadcasted_iota(jnp.int32, (128, UNIT), 0) == (flat & 127)
        found = jnp.dot(both, jnp.where(lane, 1.0, 0.0).astype(BF16), preferred_element_type=F32)
        row = lax.broadcasted_iota(jnp.int32, (16, UNIT), 0) == (flat >> 7)
        value = jnp.where(row, found[0:16] * 64.0 + found[16:32], 0.0)
        lines.append(jnp.sum(value, axis=0, keepdims=True))
    return jnp.concatenate(lines, axis=1).astype(jnp.int32)


def selector(colour, u, half):
    flat = flat_place(lax.broadcasted_iota(jnp.int32, (128, 128), 0) + half * 64, colour, u)
    lane = lax.broadcasted_iota(jnp.int32, (128, 128), 1) == (flat & 127)
    return jnp.where(lane, 1.0, 0.0).astype(BF16)


def in_order(loss, select, colour, u):
    total = None
    for half in range(2):
        l = lax.broadcasted_iota(jnp.int32, (16, 128), 1) + half * 64
        here = lax.broadcasted_iota(jnp.int32, (16, 128), 0) == (flat_place(l, colour, u) >> 7)
        here = here & (l >= half * 128)
        parts = [jnp.where(here, part.astype(F32), 0.0).astype(BF16) for part in exact_parts(loss[half : half + 1])]
        found = jnp.dot(jnp.concatenate(parts, axis=0), select[half], preferred_element_type=F32)
        total = found if total is None else total + found
    return (total[0:16] + total[16:32]) + total[32:48]


def scored_batch(c_buf, q_ref, t_ref, first, cols, s0, s1):
    rows = s0.shape[0]
    blocks = c_buf.shape[0] // rows
    groups = rows // 8
    q_rows = pl.ds(first, cols)
    wanted = jnp.broadcast_to(t_ref[:, first : first + cols], (8, cols))
    wanted = wanted - lax.broadcasted_iota(jnp.int32, (8, cols), 0)

    def scored(k, held):
        part = c_buf[pl.ds(pl.multiple_of(k * rows, rows), rows), :]
        scores = lax.dot_general(part, q_ref[q_rows, :], (((1,), (1,)), ((), ())), preferred_element_type=F32)
        held[...] = scores
        return scores

    def peak(scores, top):
        return jnp.maximum(top, jnp.max(scores.reshape(groups, 8, cols), axis=0))

    def take(held, k, old, new, total, picked):
        total = total * jnp.exp(old - new)
        for g in range(groups):
            value = held[g * 8 : (g + 1) * 8, :]
            total = total + jnp.exp(value - new)
            picked = jnp.where(wanted == k * rows + g * 8, value, picked)
        return total, picked

    def step(j, carry):
        old, new, total, picked = carry
        newer = peak(scored(2 * j + 1, s1), new)
        total, picked = take(s0, 2 * j, old, new, total, picked)
        newest = peak(scored(2 * j + 2, s0), newer)
        total, picked = take(s1, 2 * j + 1, new, newer, total, picked)
        return newer, newest, total, picked

    old = jnp.full((8, cols), LOW, F32)
    zero = jnp.zeros((8, cols), F32)
    carry = (old, peak(scored(0, s0), old), zero, zero)
    old, new, total, picked = lax.fori_loop(0, blocks // 2 - 1, step, carry)
    newer = peak(scored(blocks - 1, s1), new)
    total, picked = take(s0, blocks - 2, old, new, total, picked)
    total, picked = take(s1, blocks - 1, new, newer, total, picked)
    top = jnp.max(newer, axis=0, keepdims=True)
    total = jnp.sum(total * jnp.exp(newer - top), axis=0, keepdims=True)
    return top, total, jnp.sum(picked, axis=0, keepdims=True)


def loss_kernel(
    q_hbm, c_hbm, t_hbm, o_ref, mean_ref,
    t_nat, t_ref, select, c_buf, all_ref, first, narrow0, narrow1, wide0, wide1,
    partial, from_row, at_y, from_y, at_z, from_z, shared,
    small, loaded, send1, recv1, send2, recv2, send3, recv3, sendp, recvp, sends, recvs,
):
    z, u, v, c = place()
    x = v * (1 - c) + u * c
    y = u * (1 - c) + v * c

    def device(z, x, y, c):
        return (z, (x * 4 + y) * 2 + c)

    chunk = c_buf.shape[0] // loaded.shape[0]
    loads = [
        pltpu.make_async_copy(c_hbm.at[pl.ds(i * chunk, chunk)], c_buf.at[pl.ds(i * chunk, chunk)], loaded.at[i])
        for i in range(loaded.shape[0])
    ]
    ask = pltpu.make_async_copy(q_hbm, first.at[z], small.at[0])
    ask_t = pltpu.make_async_copy(t_hbm, t_nat, small.at[1])
    ask.start()
    ask_t.start()
    partner = device(z, x, y, 1 - c)
    column = [device((z + d) % 8, x, y, c) for d in range(1, 8)]
    xs = [device(z, (x + d) % 4, y, c) for d in range(1, 4)]
    ys = [device(z, x, (y + d) % 4, c) for d in range(1, 4)]
    crossed = [device(z, (x + d) % 4, y, 1 - c) for d in range(1, 4)]
    along_v = {d: at(z, u, (v + d) % 4, c) for d in NEAR_FIRST}
    along_u = {d: at(z, (u + d) % 4, v, c) for d in NEAR_FIRST}
    meet(column + xs + ys + crossed + [partner])
    for load in loads:
        load.start()
    ask.wait()
    sent = []

    def copy(src, dst, send, recv, to):
        return pltpu.make_async_remote_copy(
            src_ref=src, dst_ref=dst, send_sem=send, recv_sem=recv, device_id=to, device_id_type=MESH
        )

    def start(*args):
        one = copy(*args)
        one.start()
        sent.append(one)

    for d in (4, 3, 5, 2, 6, 1, 7):
        start(first.at[z], first.at[z], send1.at[d], recv1.at[d], column[d - 1])
    slots = [None] * 8
    for far in range(4):
        slots[OWN[far]] = c, (u + far) % 4
        slots[OTHER[far]] = 1 - c, (v + far) % 4
    ask_t.wait()
    owner = z * 32 + lax.axis_index("shard")
    t_ref[...] = own_targets(t_nat[...], owner, c_buf.shape[0], slots)
    for half in range(2):
        select[half] = selector(c, x, half)
    for d in (1, 7, 2, 6, 3, 5, 4):
        here = first.at[(z + 8 - d) % 8]
        copy(here, here, send1.at[d], recv1.at[d], column[d - 1]).wait_recv()
    block = jnp.concatenate([first[k].astype(F32) for k in range(8)], axis=0)
    all_ref[rows_of(0, v), :] = block.astype(BF16)

    def to_partner(far, d):
        held = all_ref.at[rows_of(OWN[far], (v + 4 - d) % 4)]
        there = all_ref.at[rows_of(OTHER[far], (v + 4 - d) % 4)]
        start(held, there, sendp.at[far, d], recvp.at[far, d], partner)

    def along(e, d):
        held = all_ref.at[rows_of(0, (v + 4 - d) % 4)]
        there = all_ref.at[rows_of(OWN[(4 - e) % 4], (v + 4 - d) % 4)]
        start(held, there, send3.at[e, d], recv3.at[e, d], along_u[e])

    def arrived_along(e, d):
        here = all_ref.at[rows_of(OWN[(4 - e) % 4], (v + 4 - d) % 4)]
        copy(here, here, send3.at[e, d], recv3.at[e, d], along_u[e]).wait_recv()

    def from_partner(far):
        for d in range(4):
            here = all_ref.at[rows_of(OTHER[far], (u + 4 - d) % 4)]
            copy(here, here, sendp.at[far, d], recvp.at[far, d], partner).wait_recv()

    own = all_ref.at[rows_of(0, v)]
    for d in (2, 1, 3):
        start(own, own, send2.at[d], recv2.at[d], along_v[d])
    to_partner(0, 0)
    along(1, 0)
    along(3, 0)
    for d in NEAR_FIRST:
        here = all_ref.at[rows_of(0, (v + 4 - d) % 4)]
        copy(here, here, send2.at[d], recv2.at[d], along_v[d]).wait_recv()
        to_partner(0, d)
        along(1, d)
        along(3, d)
    for load in loads:
        load.wait()
    from_partner(0)

    results = []

    def run(k):
        begin, cols = BATCHES[k]
        held = (narrow0, narrow1) if cols == narrow0.shape[1] else (wide0, wide1)
        results.append(scored_batch(c_buf, all_ref, t_ref, begin, cols, *held))

    run(0)
    for d in (0, 1, 3, 2):
        for e in (1, 3):
            arrived_along(e, d)
            if e == RELAYED_BY[d]:
                held = all_ref.at[rows_of(OWN[(4 - e) % 4], (v + 4 - d) % 4)]
                there = all_ref.at[rows_of(OWN[2], (v + 4 - d) % 4)]
                start(held, there, send3.at[2, d], recv3.at[2, d], along_u[e])
            to_partner((4 - e) % 4, d)
    run(1)
    for d in (0, 1, 3, 2):
        arrived_along(2, d)
        to_partner(2, d)
    from_partner(1)
    from_partner(3)
    run(2)
    from_partner(2)
    run(3)

    lines = [jnp.concatenate(parts, axis=1) for parts in zip(*results)]
    for slot, (colour, there) in enumerate(slots):
        parts = []
        for line in lines:
            parts.append(line[:, slot * UNIT : slot * UNIT + 128])
            parts.append(line[:, slot * UNIT + 64 : slot * UNIT + 192])
        partial[colour * 4 + there] = jnp.concatenate(parts + [jnp.zeros((2, 128), F32)], axis=0)

    def pass_on(k, src, dst, to):
        start(src, dst, sends.at[k], recvs.at[k], to)

    def wait(k, here):
        copy(here, here, sends.at[k], recvs.at[k], partner).wait_recv()

    unit = c * 4 + x
    row = [None] + [((x + k // 2) % 4, (c + k) % 2) for k in range(1, 8)]
    for k in (4, 5, 2, 3, 6, 7, 1):
        there, core = row[k]
        pass_on(13 + k, partial.at[core * 4 + there], from_row.at[k], device(z, there, y, core))
    for k in range(1, 8):
        wait(13 + k, from_row.at[k])
    at_y[...] = combined([partial[unit]] + [from_row[k] for k in range(1, 8)])
    for d in range(1, 4):
        pass_on(3 + d, at_y, from_y.at[d], ys[d - 1])
    for d in range(1, 4):
        wait(3 + d, from_y.at[d])
    at_z[...] = combined([at_y[...]] + [from_y[d] for d in range(1, 4)])
    for d in (4, 3, 5, 2, 6, 1, 7):
        pass_on(6 + d, at_z, from_z.at[d], column[d - 1])
    for d in range(1, 8):
        wait(6 + d, from_z.at[d])
    whole = combined([at_z[...]] + [from_z[d] for d in range(1, 8)])
    loss = whole[0:2] + jnp.log(whole[2:4]) - whole[4:6]
    shared[0] = in_order(loss, select, c, x)
    for k in (4, 5, 2, 3, 6, 7, 1):
        there, core = row[k]
        pass_on(20 + k, shared.at[0], shared.at[k], device(z, there, y, core))
    for k in range(1, 8):
        wait(20 + k, shared.at[k])
    every = ((shared[0] + shared[1]) + (shared[2] + shared[3])) + ((shared[4] + shared[5]) + (shared[6] + shared[7]))
    o_ref[...] = every[0:12]
    mean_ref[...] = jnp.sum(every, keepdims=True) * (1.0 / (8 * UNIT))
    for one in sent:
        one.wait_send()


def all_losses(queries, candidates, targets):
    count, width = candidates.shape
    tile = (8, 128)
    dma = pltpu.SemaphoreType.DMA
    return pl.pallas_call(
        loss_kernel,
        out_shape=(jax.ShapeDtypeStruct((12, 128), F32), jax.ShapeDtypeStruct((1, 1), F32)),
        in_specs=[
            pl.BlockSpec(memory_space=pltpu.HBM),
            pl.BlockSpec(memory_space=pltpu.HBM),
            pl.BlockSpec(memory_space=pltpu.HBM),
        ],
        out_specs=(pl.BlockSpec(memory_space=pltpu.VMEM), pl.BlockSpec(memory_space=pltpu.VMEM)),
        scratch_shapes=[
            pltpu.VMEM((12, 128), jnp.int32),
            pltpu.VMEM((1, 8 * UNIT), jnp.int32),
            pltpu.VMEM((2, 128, 128), BF16),
            pltpu.VMEM((count, width), BF16),
            pltpu.VMEM((8 * UNIT, width), BF16),
            pltpu.VMEM((8, PER, width), BF16),
            pltpu.VMEM((1024, 256), F32),
            pltpu.VMEM((1024, 256), F32),
            pltpu.VMEM((512, 512), F32),
            pltpu.VMEM((512, 512), F32),
            pltpu.VMEM((8, *tile), F32),
            pltpu.VMEM((8, *tile), F32),
            pltpu.VMEM(tile, F32),
            pltpu.VMEM((4, *tile), F32),
            pltpu.VMEM(tile, F32),
            pltpu.VMEM((8, *tile), F32),
            pltpu.VMEM((8, 16, 128), F32),
        ]
        + [dma((2,)), dma((4,)), dma((8,)), dma((8,)), dma((4,)), dma((4,)), dma((4, 4)), dma((4, 4)), dma((4, 4)), dma((4, 4))]
        + [dma((28,)), dma((28,))],
        compiler_params=pltpu.CompilerParams(
            collective_id=1, has_side_effects=True, vmem_limit_bytes=67_043_328
        ),
        name="ranking_losses",
    )(queries, candidates, targets)


def combined(tiles):
    tops = [tile[0:2] for tile in tiles]
    top = functools.reduce(jnp.maximum, tops)
    total = sum(tile[2:4] * jnp.exp(one - top) for tile, one in zip(tiles, tops))
    picked = sum(tile[4:6] for tile in tiles)
    return jnp.concatenate([top, total, picked, jnp.zeros((2, 128), F32)], axis=0)


def on_device(queries, candidates, targets):
    losses, mean = all_losses(queries, candidates, targets.reshape(12, 128))
    return losses.reshape(-1), mean[0, 0]


def solution(mesh):
    whole = P(("group", "shard"), None)
    return jax.shard_map(
        on_device, mesh=mesh, in_specs=(whole, whole, P()), out_specs=(P(), P()), check_vma=False
    )
```

```python
import functools

import jax
import jax.numpy as jnp
from jax import lax
from jax.experimental import pallas as pl
from jax.experimental.pallas import tpu as pltpu
from jax.sharding import PartitionSpec as P

F32 = jnp.float32
BF16 = jnp.bfloat16
MESH = pl.DeviceIdType.MESH
LOW = -3.0e38
PER = 6
BLOCK = 48
UNIT = 192
NEAR_FIRST = (1, 3, 2)
RELAYED_BY = (1, 3, None, 1)
BATCHES = ((0, 256), (256, 512), (768, 512), (1280, 256))


def place():
    z = lax.axis_index("group")
    s = lax.axis_index("shard")
    x, y, c = s // 8, (s // 2) % 4, s % 2
    u = y * (1 - c) + x * c
    v = x * (1 - c) + y * c
    return z, u, v, c


def at(z, u, v, c):
    x = v * (1 - c) + u * c
    y = u * (1 - c) + v * c
    return (z, (x * 4 + y) * 2 + c)


def own_slot(far, c):
    return {0: 0, 1: 4 - 2 * c, 3: 5 - 2 * c, 2: 6}[far]


def other_slot(far, c):
    return {0: 1, 1: 2 + 2 * c, 3: 3 + 2 * c, 2: 7}[far]


def rows_of(slot, v):
    return pl.ds(pl.multiple_of(slot * UNIT + v * BLOCK, 16), BLOCK)


def meet(others):
    barrier = pltpu.get_barrier_semaphore()
    for other in others:
        pl.semaphore_signal(barrier, inc=1, device_id=other, device_id_type=MESH)
    pl.semaphore_wait(barrier, len(others))


def flat_place(l, colour, u):
    v = (l * 1366) >> 16
    l = l - v * BLOCK
    z = (l * 10923) >> 16
    r = l - z * PER
    chip = v * (4 - 3 * colour) + u * (1 + 3 * colour)
    return z * UNIT + chip * 2 * PER + colour * PER + r


def exact_parts(a):
    high = a.astype(BF16)
    rest = a - high.astype(F32)
    middle = rest.astype(BF16)
    return high, middle, (rest - middle.astype(F32)).astype(BF16)


def own_targets(targets, owner, rows, slots):
    local = targets - owner * rows
    local = jnp.where((local >= 0) & (local < rows), local, rows)
    pad = jnp.zeros((4, 128), jnp.int32)
    both = jnp.concatenate([local >> 6, pad, local & 63, pad], axis=0).astype(F32).astype(BF16)
    lines = []
    for colour, u in slots:
        flat = flat_place(lax.broadcasted_iota(jnp.int32, (1, UNIT), 1), colour, u)
        lane = lax.broadcasted_iota(jnp.int32, (128, UNIT), 0) == (flat & 127)
        found = jnp.dot(both, jnp.where(lane, 1.0, 0.0).astype(BF16), preferred_element_type=F32)
        row = lax.broadcasted_iota(jnp.int32, (16, UNIT), 0) == (flat >> 7)
        value = jnp.where(row, found[0:16] * 64.0 + found[16:32], 0.0)
        lines.append(jnp.sum(value, axis=0, keepdims=True))
    return jnp.concatenate(lines, axis=1).astype(jnp.int32)


def selector(colour, u, half):
    flat = flat_place(lax.broadcasted_iota(jnp.int32, (128, 128), 0) + half * 64, colour, u)
    lane = lax.broadcasted_iota(jnp.int32, (128, 128), 1) == (flat & 127)
    return jnp.where(lane, 1.0, 0.0).astype(BF16)


def in_order(loss, select, colour, u):
    total = None
    for half in range(2):
        l = lax.broadcasted_iota(jnp.int32, (16, 128), 1) + half * 64
        here = lax.broadcasted_iota(jnp.int32, (16, 128), 0) == (flat_place(l, colour, u) >> 7)
        here = here & (l >= half * 128)
        parts = [jnp.where(here, part.astype(F32), 0.0).astype(BF16) for part in exact_parts(loss[half : half + 1])]
        found = jnp.dot(jnp.concatenate(parts, axis=0), select[half], preferred_element_type=F32)
        total = found if total is None else total + found
    return (total[0:16] + total[16:32]) + total[32:48]


def scored_batch(c_buf, q_ref, t_ref, first, cols, s0, s1, between):
    rows = s0.shape[0]
    blocks = c_buf.shape[0] // rows
    groups = rows // 8
    q_rows = pl.ds(first, cols)
    wanted = jnp.broadcast_to(t_ref[:, first : first + cols], (8, cols))
    wanted = wanted - lax.broadcasted_iota(jnp.int32, (8, cols), 0)

    def scored(k, held):
        part = c_buf[pl.ds(pl.multiple_of(k * rows, rows), rows), :]
        scores = lax.dot_general(part, q_ref[q_rows, :], (((1,), (1,)), ((), ())), preferred_element_type=F32)
        held[...] = scores
        return scores

    def peak(scores, top):
        return jnp.maximum(top, jnp.max(scores.reshape(groups, 8, cols), axis=0))

    def take(held, k, old, new, total, picked):
        total = total * jnp.exp(old - new)
        for g in range(groups):
            value = held[g * 8 : (g + 1) * 8, :]
            total = total + jnp.exp(value - new)
            picked = jnp.where(wanted == k * rows + g * 8, value, picked)
        return total, picked

    def step(j, carry):
        old, new, total, picked = carry
        newer = peak(scored(2 * j + 1, s1), new)
        total, picked = take(s0, 2 * j, old, new, total, picked)
        newest = peak(scored(2 * j + 2, s0), newer)
        total, picked = take(s1, 2 * j + 1, new, newer, total, picked)
        return newer, newest, total, picked

    old = jnp.full((8, cols), LOW, F32)
    zero = jnp.zeros((8, cols), F32)
    carry = (old, peak(scored(0, s0), old), zero, zero)
    pairs = blocks // 2 - 1
    for k, handle in enumerate(between):
        if handle is not None:
            handle()
        if k < pairs:
            carry = lax.fori_loop(k, k + 1, step, carry)
    carry = lax.fori_loop(min(len(between), pairs), pairs, step, carry)
    old, new, total, picked = carry
    newer = peak(scored(blocks - 1, s1), new)
    total, picked = take(s0, blocks - 2, old, new, total, picked)
    total, picked = take(s1, blocks - 1, new, newer, total, picked)
    top = jnp.max(newer, axis=0, keepdims=True)
    total = jnp.sum(total * jnp.exp(newer - top), axis=0, keepdims=True)
    return top, total, jnp.sum(picked, axis=0, keepdims=True)


def loss_kernel(
    q_hbm, c_hbm, t_hbm, o_ref, mean_ref,
    t_nat, t_ref, select, c_buf, all_ref, first, narrow0, narrow1, wide0, wide1,
    partial, from_row, at_y, from_y, at_z, from_z, shared,
    small, loaded, send1, recv1, send2, recv2, send3, recv3, sendp, recvp, sends, recvs,
):
    z, u, v, c = place()
    x = v * (1 - c) + u * c
    y = u * (1 - c) + v * c

    def device(z, x, y, c):
        return (z, (x * 4 + y) * 2 + c)

    chunk = c_buf.shape[0] // loaded.shape[0]
    loads = [
        pltpu.make_async_copy(c_hbm.at[pl.ds(i * chunk, chunk)], c_buf.at[pl.ds(i * chunk, chunk)], loaded.at[i])
        for i in range(loaded.shape[0])
    ]
    ask = pltpu.make_async_copy(q_hbm, first.at[z], small.at[0])
    ask_t = pltpu.make_async_copy(t_hbm, t_nat, small.at[1])
    ask.start()
    ask_t.start()
    partner = device(z, x, y, 1 - c)
    column = [device((z + d) % 8, x, y, c) for d in range(1, 8)]
    xs = [device(z, (x + d) % 4, y, c) for d in range(1, 4)]
    ys = [device(z, x, (y + d) % 4, c) for d in range(1, 4)]
    crossed = [device(z, (x + d) % 4, y, 1 - c) for d in range(1, 4)]
    along_v = {d: at(z, u, (v + d) % 4, c) for d in NEAR_FIRST}
    along_u = {d: at(z, (u + d) % 4, v, c) for d in NEAR_FIRST}
    meet(column + xs + ys + crossed + [partner])
    for load in loads:
        load.start()
    ask.wait()

    def copy(src, dst, send, recv, to):
        return pltpu.make_async_remote_copy(
            src_ref=src, dst_ref=dst, send_sem=send, recv_sem=recv, device_id=to, device_id_type=MESH
        )

    def start(*args):
        copy(*args).start()

    for d in (4, 3, 5, 2, 6, 1, 7):
        start(first.at[z], first.at[z], send1.at[d], recv1.at[d], column[d - 1])
    slots = [(c, u), (1 - c, v), (1, (x + 1) % 4), (1, (x + 3) % 4)]
    slots += [(0, (y + 1) % 4), (0, (y + 3) % 4), (c, (u + 2) % 4), (1 - c, (v + 2) % 4)]
    ask_t.wait()
    owner = z * 32 + lax.axis_index("shard")
    t_ref[...] = own_targets(t_nat[...], owner, c_buf.shape[0], slots)
    for half in range(2):
        select[half] = selector(c, x, half)
    for d in (1, 7, 2, 6, 3, 5, 4):
        here = first.at[(z + 8 - d) % 8]
        copy(here, here, send1.at[d], recv1.at[d], column[d - 1]).wait_recv()
    block = jnp.concatenate([first[k].astype(F32) for k in range(8)], axis=0)
    all_ref[rows_of(0, v), :] = block.astype(BF16)

    def to_partner(far, d):
        held = all_ref.at[rows_of(own_slot(far, c), (v + 4 - d) % 4)]
        there = all_ref.at[rows_of(other_slot(far, 1 - c), (v + 4 - d) % 4)]
        start(held, there, sendp.at[far, d], recvp.at[far, d], partner)

    def along(e, d):
        held = all_ref.at[rows_of(0, (v + 4 - d) % 4)]
        there = all_ref.at[rows_of(own_slot((4 - e) % 4, c), (v + 4 - d) % 4)]
        start(held, there, send3.at[e, d], recv3.at[e, d], along_u[e])

    def arrived_along(e, d):
        here = all_ref.at[rows_of(own_slot((4 - e) % 4, c), (v + 4 - d) % 4)]
        copy(here, here, send3.at[e, d], recv3.at[e, d], along_u[e]).wait_recv()

    def from_partner(far):
        for d in range(4):
            here = all_ref.at[rows_of(other_slot(far, c), (u + 4 - d) % 4)]
            copy(here, here, sendp.at[far, d], recvp.at[far, d], partner).wait_recv()

    own = all_ref.at[rows_of(0, v)]
    for d in (2, 1, 3):
        start(own, own, send2.at[d], recv2.at[d], along_v[d])
    to_partner(0, 0)
    along(1, 0)
    along(3, 0)
    for d in NEAR_FIRST:
        here = all_ref.at[rows_of(0, (v + 4 - d) % 4)]
        copy(here, here, send2.at[d], recv2.at[d], along_v[d]).wait_recv()
        to_partner(0, d)
        along(1, d)
        along(3, d)
    along(2, 2)

    def near_blocks(*ds):
        for d in ds:
            for e in (1, 3):
                arrived_along(e, d)
                if e == RELAYED_BY[d]:
                    held = all_ref.at[rows_of(own_slot((4 - e) % 4, c), (v + 4 - d) % 4)]
                    there = all_ref.at[rows_of(own_slot(2, c), (v + 4 - d) % 4)]
                    start(held, there, send3.at[2, d], recv3.at[2, d], along_u[e])
                to_partner((4 - e) % 4, d)

    def on_core(core, handle, *ds):
        pl.when(c == core)(lambda: handle(*ds))

    def near_from_partner():
        from_partner(1)
        from_partner(3)

    on_core(1, near_blocks, 0, 1, 3, 2)
    on_core(0, near_blocks, 0)
    for load in loads:
        load.wait()
    from_partner(0)

    results = []

    def run(k, between=()):
        begin, cols = BATCHES[k]
        held = (narrow0, narrow1) if cols == narrow0.shape[1] else (wide0, wide1)
        results.append(scored_batch(c_buf, all_ref, t_ref, begin, cols, *held, between))

    run(0)
    on_core(0, near_blocks, 1)
    on_core(0, near_from_partner)
    run(1, (None, lambda: on_core(0, near_blocks, 3), lambda: on_core(0, near_blocks, 2)))
    for d in (0, 1, 3, 2):
        arrived_along(2, d)
        to_partner(2, d)
    on_core(1, near_from_partner)
    run(2, (None, None, None))
    from_partner(2)
    run(3)

    lines = [jnp.concatenate(parts, axis=1) for parts in zip(*results)]
    for slot, (colour, there) in enumerate(slots):
        parts = []
        for line in lines:
            parts.append(line[:, slot * UNIT : slot * UNIT + 128])
            parts.append(line[:, slot * UNIT + 64 : slot * UNIT + 192])
        partial[colour * 4 + there] = jnp.concatenate(parts + [jnp.zeros((2, 128), F32)], axis=0)

    def pass_on(k, src, dst, to):
        start(src, dst, sends.at[k], recvs.at[k], to)

    def wait(k, here):
        copy(here, here, sends.at[k], recvs.at[k], partner).wait_recv()

    unit = c * 4 + x
    row = [None] + [((x + k // 2) % 4, (c + k) % 2) for k in range(1, 8)]
    for k in (4, 5, 2, 3, 6, 7, 1):
        there, core = row[k]
        pass_on(13 + k, partial.at[core * 4 + there], from_row.at[k], device(z, there, y, core))
    for k in range(1, 8):
        wait(13 + k, from_row.at[k])
    at_y[...] = combined([partial[unit]] + [from_row[k] for k in range(1, 8)])
    for d in range(1, 4):
        pass_on(3 + d, at_y, from_y.at[d], ys[d - 1])
    for d in range(1, 4):
        wait(3 + d, from_y.at[d])
    at_z[...] = combined([at_y[...]] + [from_y[d] for d in range(1, 4)])
    for d in (4, 3, 5, 2, 6, 1, 7):
        pass_on(6 + d, at_z, from_z.at[d], column[d - 1])
    for d in range(1, 8):
        wait(6 + d, from_z.at[d])
    whole = combined([at_z[...]] + [from_z[d] for d in range(1, 8)])
    loss = whole[0:2] + jnp.log(whole[2:4]) - whole[4:6]
    shared[0] = in_order(loss, select, c, x)
    for k in (4, 5, 2, 3, 6, 7, 1):
        there, core = row[k]
        pass_on(20 + k, shared.at[0], shared.at[k], device(z, there, y, core))
    for k in range(1, 8):
        wait(20 + k, shared.at[k])
    every = ((shared[0] + shared[1]) + (shared[2] + shared[3])) + ((shared[4] + shared[5]) + (shared[6] + shared[7]))
    o_ref[...] = every[0:12]
    mean_ref[...] = jnp.sum(every, keepdims=True) * (1.0 / (8 * UNIT))
    for d in range(1, 8):
        copy(first.at[z], first.at[z], send1.at[d], recv1.at[d], partner).wait_send()
    for d in range(4):
        if d:
            copy(own, own, send2.at[d], recv2.at[d], partner).wait_send()
        for e in range(4):
            copy(own, own, sendp.at[e, d], recvp.at[e, d], partner).wait_send()
            if e:
                copy(own, own, send3.at[e, d], recv3.at[e, d], partner).wait_send()
    for k in range(1, 8):
        if k < 4:
            copy(at_y, at_y, sends.at[3 + k], recvs.at[3 + k], partner).wait_send()
        copy(at_z, at_z, sends.at[6 + k], recvs.at[6 + k], partner).wait_send()
        copy(at_z, at_z, sends.at[13 + k], recvs.at[13 + k], partner).wait_send()
        copy(shared.at[0], shared.at[0], sends.at[20 + k], recvs.at[20 + k], partner).wait_send()


def all_losses(queries, candidates, targets):
    count, width = candidates.shape
    tile = (8, 128)
    dma = pltpu.SemaphoreType.DMA
    return pl.pallas_call(
        loss_kernel,
        out_shape=(jax.ShapeDtypeStruct((12, 128), F32), jax.ShapeDtypeStruct((1, 1), F32)),
        in_specs=[
            pl.BlockSpec(memory_space=pltpu.HBM),
            pl.BlockSpec(memory_space=pltpu.HBM),
            pl.BlockSpec(memory_space=pltpu.HBM),
        ],
        out_specs=(pl.BlockSpec(memory_space=pltpu.VMEM), pl.BlockSpec(memory_space=pltpu.VMEM)),
        scratch_shapes=[
            pltpu.VMEM((12, 128), jnp.int32),
            pltpu.VMEM((1, 8 * UNIT), jnp.int32),
            pltpu.VMEM((2, 128, 128), BF16),
            pltpu.VMEM((count, width), BF16),
            pltpu.VMEM((8 * UNIT, width), BF16),
            pltpu.VMEM((8, PER, width), BF16),
            pltpu.VMEM((1024, 256), F32),
            pltpu.VMEM((1024, 256), F32),
            pltpu.VMEM((512, 512), F32),
            pltpu.VMEM((512, 512), F32),
            pltpu.VMEM((8, *tile), F32),
            pltpu.VMEM((8, *tile), F32),
            pltpu.VMEM(tile, F32),
            pltpu.VMEM((4, *tile), F32),
            pltpu.VMEM(tile, F32),
            pltpu.VMEM((8, *tile), F32),
            pltpu.VMEM((8, 16, 128), F32),
        ]
        + [dma((2,)), dma((4,)), dma((8,)), dma((8,)), dma((4,)), dma((4,)), dma((4, 4)), dma((4, 4)), dma((4, 4)), dma((4, 4))]
        + [dma((28,)), dma((28,))],
        compiler_params=pltpu.CompilerParams(
            collective_id=1, has_side_effects=True, vmem_limit_bytes=50 << 20
        ),
        name="ranking_losses",
    )(queries, candidates, targets)


def combined(tiles):
    tops = [tile[0:2] for tile in tiles]
    top = functools.reduce(jnp.maximum, tops)
    total = sum(tile[2:4] * jnp.exp(one - top) for tile, one in zip(tiles, tops))
    picked = sum(tile[4:6] for tile in tiles)
    return jnp.concatenate([top, total, picked, jnp.zeros((2, 128), F32)], axis=0)


def on_device(queries, candidates, targets):
    held = (queries, candidates, targets.reshape(12, 128))
    losses, mean = all_losses(*(pltpu.with_memory_space_constraint(a, pltpu.HBM) for a in held))
    return losses.reshape(-1), mean[0, 0]


def solution(mesh):
    whole = P(("group", "shard"), None)
    return jax.shard_map(
        on_device, mesh=mesh, in_specs=(whole, whole, P()), out_specs=(P(), P()), check_vma=False
    )
```

```python
import functools

import jax
import jax.numpy as jnp
from jax import lax
from jax.experimental import pallas as pl
from jax.experimental.pallas import tpu as pltpu
from jax.sharding import PartitionSpec as P

F32 = jnp.float32
BF16 = jnp.bfloat16
MESH = pl.DeviceIdType.MESH
LOW = -3.0e38
PER = 6
BLOCK = 48
UNIT = 192
NEAR_FIRST = (1, 3, 2)
RELAYED_BY = (1, 3, None, 1)
BATCHES = ((0, 256), (256, 512), (768, 512), (1280, 256))


def place():
    z = lax.axis_index("group")
    s = lax.axis_index("shard")
    x, y, c = s // 8, (s // 2) % 4, s % 2
    u = y * (1 - c) + x * c
    v = x * (1 - c) + y * c
    return z, u, v, c


def at(z, u, v, c):
    x = v * (1 - c) + u * c
    y = u * (1 - c) + v * c
    return (z, (x * 4 + y) * 2 + c)


def own_slot(far, c):
    return {0: 0, 1: 4 - 2 * c, 3: 5 - 2 * c, 2: 6}[far]


def other_slot(far, c):
    return {0: 1, 1: 2 + 2 * c, 3: 3 + 2 * c, 2: 7}[far]


def rows_of(slot, v):
    return pl.ds(pl.multiple_of(slot * UNIT + v * BLOCK, 16), BLOCK)


def meet(others):
    barrier = pltpu.get_barrier_semaphore()
    for other in others:
        pl.semaphore_signal(barrier, inc=1, device_id=other, device_id_type=MESH)
    pl.semaphore_wait(barrier, len(others))


def flat_place(l, colour, u):
    v = (l * 1366) >> 16
    l = l - v * BLOCK
    z = (l * 10923) >> 16
    r = l - z * PER
    chip = v * (4 - 3 * colour) + u * (1 + 3 * colour)
    return z * UNIT + chip * 2 * PER + colour * PER + r


def exact_parts(a):
    high = a.astype(BF16)
    rest = a - high.astype(F32)
    middle = rest.astype(BF16)
    return high, middle, (rest - middle.astype(F32)).astype(BF16)


def own_targets(targets, owner, rows, slots):
    local = targets - owner * rows
    local = jnp.where((local >= 0) & (local < rows), local, rows)
    pad = jnp.zeros((4, 128), jnp.int32)
    both = jnp.concatenate([local >> 6, pad, local & 63, pad], axis=0).astype(F32).astype(BF16)
    lines = []
    for colour, u in slots:
        flat = flat_place(lax.broadcasted_iota(jnp.int32, (1, UNIT), 1), colour, u)
        lane = lax.broadcasted_iota(jnp.int32, (128, UNIT), 0) == (flat & 127)
        found = jnp.dot(both, jnp.where(lane, 1.0, 0.0).astype(BF16), preferred_element_type=F32)
        row = lax.broadcasted_iota(jnp.int32, (16, UNIT), 0) == (flat >> 7)
        value = jnp.where(row, found[0:16] * 64.0 + found[16:32], 0.0)
        lines.append(jnp.sum(value, axis=0, keepdims=True))
    return jnp.concatenate(lines, axis=1).astype(jnp.int32)


def selector(colour, u, half):
    flat = flat_place(lax.broadcasted_iota(jnp.int32, (128, 128), 0) + half * 64, colour, u)
    lane = lax.broadcasted_iota(jnp.int32, (128, 128), 1) == (flat & 127)
    return jnp.where(lane, 1.0, 0.0).astype(BF16)


def in_order(loss, select, colour, u):
    total = None
    for half in range(2):
        l = lax.broadcasted_iota(jnp.int32, (16, 128), 1) + half * 64
        here = lax.broadcasted_iota(jnp.int32, (16, 128), 0) == (flat_place(l, colour, u) >> 7)
        here = here & (l >= half * 128)
        parts = [jnp.where(here, part.astype(F32), 0.0).astype(BF16) for part in exact_parts(loss[half : half + 1])]
        found = jnp.dot(jnp.concatenate(parts, axis=0), select[half], preferred_element_type=F32)
        total = found if total is None else total + found
    return (total[0:16] + total[16:32]) + total[32:48]


def scored_batch(c_buf, q_ref, t_ref, first, cols, s0, s1, between, before):
    rows = s0.shape[0]
    blocks = c_buf.shape[0] // rows
    groups = rows // 8
    q_rows = pl.ds(first, cols)
    wanted = jnp.broadcast_to(t_ref[:, first : first + cols], (8, cols))
    wanted = wanted - lax.broadcasted_iota(jnp.int32, (8, cols), 0)

    def scored(k, held):
        part = c_buf[pl.ds(pl.multiple_of(k * rows, rows), rows), :]
        scores = lax.dot_general(part, q_ref[q_rows, :], (((1,), (1,)), ((), ())), preferred_element_type=F32)
        held[...] = scores
        return scores

    def peak(scores, top):
        return jnp.maximum(top, jnp.max(scores.reshape(groups, 8, cols), axis=0))

    def take(held, k, old, new, total, picked):
        total = total * jnp.exp(old - new)
        for g in range(groups):
            value = held[g * 8 : (g + 1) * 8, :]
            total = total + jnp.exp(value - new)
            picked = jnp.where(wanted == k * rows + g * 8, value, picked)
        return total, picked

    def step(j, carry):
        old, new, total, picked = carry
        newer = peak(scored(2 * j + 1, s1), new)
        total, picked = take(s0, 2 * j, old, new, total, picked)
        newest = peak(scored(2 * j + 2, s0), newer)
        total, picked = take(s1, 2 * j + 1, new, newer, total, picked)
        return newer, newest, total, picked

    old = jnp.full((8, cols), LOW, F32)
    zero = jnp.zeros((8, cols), F32)
    carry = (old, peak(scored(0, s0), old), zero, zero)
    before()
    pairs = blocks // 2 - 1
    for k, handle in enumerate(between):
        if handle is not None:
            handle()
        if k < pairs:
            carry = lax.fori_loop(k, k + 1, step, carry)
    carry = lax.fori_loop(min(len(between), pairs), pairs, step, carry)
    old, new, total, picked = carry
    newer = peak(scored(blocks - 1, s1), new)
    total, picked = take(s0, blocks - 2, old, new, total, picked)

    def finish():
        last, found = take(s1, blocks - 1, new, newer, total, picked)
        top = jnp.max(newer, axis=0, keepdims=True)
        last = jnp.sum(last * jnp.exp(newer - top), axis=0, keepdims=True)
        return top, last, jnp.sum(found, axis=0, keepdims=True)

    return finish


def loss_kernel(
    q_hbm, c_hbm, t_hbm, o_ref, mean_ref,
    t_nat, t_ref, select, c_buf, all_ref, first, narrow0, narrow1, wide0, wide1,
    partial, from_row, at_y, from_y, at_z, from_z, shared,
    small, loaded, send1, recv1, send2, recv2, send3, recv3, sendp, recvp, sends, recvs,
):
    z, u, v, c = place()
    x = v * (1 - c) + u * c
    y = u * (1 - c) + v * c

    def device(z, x, y, c):
        return (z, (x * 4 + y) * 2 + c)

    chunk = c_buf.shape[0] // loaded.shape[0]
    loads = [
        pltpu.make_async_copy(c_hbm.at[pl.ds(i * chunk, chunk)], c_buf.at[pl.ds(i * chunk, chunk)], loaded.at[i])
        for i in range(loaded.shape[0])
    ]
    ask = pltpu.make_async_copy(q_hbm, first.at[z], small.at[0])
    ask_t = pltpu.make_async_copy(t_hbm, t_nat, small.at[1])
    ask.start()
    ask_t.start()
    partner = device(z, x, y, 1 - c)
    column = [device((z + d) % 8, x, y, c) for d in range(1, 8)]
    xs = [device(z, (x + d) % 4, y, c) for d in range(1, 4)]
    ys = [device(z, x, (y + d) % 4, c) for d in range(1, 4)]
    crossed = [device(z, (x + d) % 4, y, 1 - c) for d in range(1, 4)]
    along_v = {d: at(z, u, (v + d) % 4, c) for d in NEAR_FIRST}
    along_u = {d: at(z, (u + d) % 4, v, c) for d in NEAR_FIRST}
    meet(column + xs + ys + crossed + [partner])
    for load in loads:
        load.start()
    ask.wait()

    def copy(src, dst, send, recv, to):
        return pltpu.make_async_remote_copy(
            src_ref=src, dst_ref=dst, send_sem=send, recv_sem=recv, device_id=to, device_id_type=MESH
        )

    def start(*args):
        copy(*args).start()

    for d in (4, 3, 5, 2, 6, 1, 7):
        start(first.at[z], first.at[z], send1.at[d], recv1.at[d], column[d - 1])
    slots = [(c, u), (1 - c, v), (1, (x + 1) % 4), (1, (x + 3) % 4)]
    slots += [(0, (y + 1) % 4), (0, (y + 3) % 4), (c, (u + 2) % 4), (1 - c, (v + 2) % 4)]
    ask_t.wait()
    owner = z * 32 + lax.axis_index("shard")
    t_ref[...] = own_targets(t_nat[...], owner, c_buf.shape[0], slots)
    for half in range(2):
        select[half] = selector(c, x, half)
    for d in (1, 7, 2, 6, 3, 5, 4):
        here = first.at[(z + 8 - d) % 8]
        copy(here, here, send1.at[d], recv1.at[d], column[d - 1]).wait_recv()
    block = jnp.concatenate([first[k].astype(F32) for k in range(8)], axis=0)
    all_ref[rows_of(0, v), :] = block.astype(BF16)

    def to_partner(far, d):
        held = all_ref.at[rows_of(own_slot(far, c), (v + 4 - d) % 4)]
        there = all_ref.at[rows_of(other_slot(far, 1 - c), (v + 4 - d) % 4)]
        start(held, there, sendp.at[far, d], recvp.at[far, d], partner)

    def along(e, d):
        held = all_ref.at[rows_of(0, (v + 4 - d) % 4)]
        there = all_ref.at[rows_of(own_slot((4 - e) % 4, c), (v + 4 - d) % 4)]
        start(held, there, send3.at[e, d], recv3.at[e, d], along_u[e])

    def arrived_along(e, d):
        here = all_ref.at[rows_of(own_slot((4 - e) % 4, c), (v + 4 - d) % 4)]
        copy(here, here, send3.at[e, d], recv3.at[e, d], along_u[e]).wait_recv()

    def from_partner(far):
        for d in range(4):
            here = all_ref.at[rows_of(other_slot(far, c), (u + 4 - d) % 4)]
            copy(here, here, sendp.at[far, d], recvp.at[far, d], partner).wait_recv()

    own = all_ref.at[rows_of(0, v)]
    for d in (2, 1, 3):
        start(own, own, send2.at[d], recv2.at[d], along_v[d])
    to_partner(0, 0)
    along(1, 0)
    along(3, 0)
    for d in NEAR_FIRST:
        here = all_ref.at[rows_of(0, (v + 4 - d) % 4)]
        copy(here, here, send2.at[d], recv2.at[d], along_v[d]).wait_recv()
        to_partner(0, d)
        along(1, d)
        along(3, d)
    along(2, 2)

    def near_blocks(*ds):
        for d in ds:
            for e in (1, 3):
                arrived_along(e, d)
                if e == RELAYED_BY[d]:
                    held = all_ref.at[rows_of(own_slot((4 - e) % 4, c), (v + 4 - d) % 4)]
                    there = all_ref.at[rows_of(own_slot(2, c), (v + 4 - d) % 4)]
                    start(held, there, send3.at[2, d], recv3.at[2, d], along_u[e])
                to_partner((4 - e) % 4, d)

    def on_core(core, handle, *ds):
        pl.when(c == core)(lambda: handle(*ds))

    def near_from_partner():
        from_partner(1)
        from_partner(3)

    on_core(1, near_blocks, 0, 1, 3, 2)
    on_core(0, near_blocks, 0)
    for load in loads:
        load.wait()
    from_partner(0)

    results = []
    ends = []

    def end():
        if ends:
            results.append(ends.pop()())

    def run(k, between=()):
        begin, cols = BATCHES[k]
        held = (narrow0, narrow1) if cols == narrow0.shape[1] else (wide0, wide1)
        ends.append(scored_batch(c_buf, all_ref, t_ref, begin, cols, *held, between, end))

    run(0)
    on_core(0, near_blocks, 1)
    on_core(0, near_from_partner)
    run(1, (None, lambda: on_core(0, near_blocks, 3), lambda: on_core(0, near_blocks, 2)))
    for d in (0, 1, 3, 2):
        arrived_along(2, d)
        to_partner(2, d)
    on_core(1, near_from_partner)
    run(2, (None, None, None))
    from_partner(2)
    run(3)
    end()

    lines = [jnp.concatenate(parts, axis=1) for parts in zip(*results)]
    for slot, (colour, there) in enumerate(slots):
        parts = []
        for line in lines:
            parts.append(line[:, slot * UNIT : slot * UNIT + 128])
            parts.append(line[:, slot * UNIT + 64 : slot * UNIT + 192])
        partial[colour * 4 + there] = jnp.concatenate(parts + [jnp.zeros((2, 128), F32)], axis=0)

    def pass_on(k, src, dst, to):
        start(src, dst, sends.at[k], recvs.at[k], to)

    def wait(k, here):
        copy(here, here, sends.at[k], recvs.at[k], partner).wait_recv()

    unit = c * 4 + x
    row = [None] + [((x + k // 2) % 4, (c + k) % 2) for k in range(1, 8)]
    for k in (4, 5, 2, 3, 6, 7, 1):
        there, core = row[k]
        pass_on(13 + k, partial.at[core * 4 + there], from_row.at[k], device(z, there, y, core))
    for k in range(1, 8):
        wait(13 + k, from_row.at[k])
    at_y[...] = combined([partial[unit]] + [from_row[k] for k in range(1, 8)])
    for d in range(1, 4):
        pass_on(3 + d, at_y, from_y.at[d], ys[d - 1])
    for d in range(1, 4):
        wait(3 + d, from_y.at[d])
    at_z[...] = combined([at_y[...]] + [from_y[d] for d in range(1, 4)])
    for d in (4, 3, 5, 2, 6, 1, 7):
        pass_on(6 + d, at_z, from_z.at[d], column[d - 1])
    for d in range(1, 8):
        wait(6 + d, from_z.at[d])
    whole = combined([at_z[...]] + [from_z[d] for d in range(1, 8)])
    loss = whole[0:2] + jnp.log(whole[2:4]) - whole[4:6]
    shared[0] = in_order(loss, select, c, x)
    for k in (4, 5, 2, 3, 6, 7, 1):
        there, core = row[k]
        pass_on(20 + k, shared.at[0], shared.at[k], device(z, there, y, core))
    for k in range(1, 8):
        wait(20 + k, shared.at[k])
    every = ((shared[0] + shared[1]) + (shared[2] + shared[3])) + ((shared[4] + shared[5]) + (shared[6] + shared[7]))
    o_ref[...] = every[0:12]
    mean_ref[...] = jnp.sum(every, keepdims=True) * (1.0 / (8 * UNIT))
    for d in range(1, 8):
        copy(first.at[z], first.at[z], send1.at[d], recv1.at[d], partner).wait_send()
    for d in range(4):
        if d:
            copy(own, own, send2.at[d], recv2.at[d], partner).wait_send()
        for e in range(4):
            copy(own, own, sendp.at[e, d], recvp.at[e, d], partner).wait_send()
            if e:
                copy(own, own, send3.at[e, d], recv3.at[e, d], partner).wait_send()
    for k in range(1, 8):
        if k < 4:
            copy(at_y, at_y, sends.at[3 + k], recvs.at[3 + k], partner).wait_send()
        copy(at_z, at_z, sends.at[6 + k], recvs.at[6 + k], partner).wait_send()
        copy(at_z, at_z, sends.at[13 + k], recvs.at[13 + k], partner).wait_send()
        copy(shared.at[0], shared.at[0], sends.at[20 + k], recvs.at[20 + k], partner).wait_send()


def all_losses(queries, candidates, targets):
    count, width = candidates.shape
    tile = (8, 128)
    dma = pltpu.SemaphoreType.DMA
    return pl.pallas_call(
        loss_kernel,
        out_shape=(jax.ShapeDtypeStruct((12, 128), F32), jax.ShapeDtypeStruct((1, 1), F32)),
        in_specs=[
            pl.BlockSpec(memory_space=pltpu.HBM),
            pl.BlockSpec(memory_space=pltpu.HBM),
            pl.BlockSpec(memory_space=pltpu.HBM),
        ],
        out_specs=(pl.BlockSpec(memory_space=pltpu.VMEM), pl.BlockSpec(memory_space=pltpu.VMEM)),
        scratch_shapes=[
            pltpu.VMEM((12, 128), jnp.int32),
            pltpu.VMEM((1, 8 * UNIT), jnp.int32),
            pltpu.VMEM((2, 128, 128), BF16),
            pltpu.VMEM((count, width), BF16),
            pltpu.VMEM((8 * UNIT, width), BF16),
            pltpu.VMEM((8, PER, width), BF16),
            pltpu.VMEM((1024, 256), F32),
            pltpu.VMEM((1024, 256), F32),
            pltpu.VMEM((512, 512), F32),
            pltpu.VMEM((512, 512), F32),
            pltpu.VMEM((8, *tile), F32),
            pltpu.VMEM((8, *tile), F32),
            pltpu.VMEM(tile, F32),
            pltpu.VMEM((4, *tile), F32),
            pltpu.VMEM(tile, F32),
            pltpu.VMEM((8, *tile), F32),
            pltpu.VMEM((8, 16, 128), F32),
        ]
        + [dma((2,)), dma((4,)), dma((8,)), dma((8,)), dma((4,)), dma((4,)), dma((4, 4)), dma((4, 4)), dma((4, 4)), dma((4, 4))]
        + [dma((28,)), dma((28,))],
        compiler_params=pltpu.CompilerParams(
            collective_id=1, has_side_effects=True, vmem_limit_bytes=50 << 20
        ),
        name="ranking_losses",
    )(queries, candidates, targets)


def combined(tiles):
    tops = [tile[0:2] for tile in tiles]
    top = functools.reduce(jnp.maximum, tops)
    total = sum(tile[2:4] * jnp.exp(one - top) for tile, one in zip(tiles, tops))
    picked = sum(tile[4:6] for tile in tiles)
    return jnp.concatenate([top, total, picked, jnp.zeros((2, 128), F32)], axis=0)


def on_device(queries, candidates, targets):
    held = (queries, candidates, targets.reshape(12, 128))
    losses, mean = all_losses(*(pltpu.with_memory_space_constraint(a, pltpu.HBM) for a in held))
    return losses.reshape(-1), mean[0, 0]


def solution(mesh):
    whole = P(("group", "shard"), None)
    return jax.shard_map(
        on_device, mesh=mesh, in_specs=(whole, whole, P()), out_specs=(P(), P()), check_vma=False
    )
```

```python
import functools

import jax
import jax.numpy as jnp
from jax import lax
from jax.experimental import pallas as pl
from jax.experimental.pallas import tpu as pltpu
from jax.sharding import PartitionSpec as P

F32 = jnp.float32
BF16 = jnp.bfloat16
MESH = pl.DeviceIdType.MESH
LOW = -3.0e38
PER = 6
BLOCK = 48
UNIT = 192
NEAR_FIRST = (1, 3, 2)
RELAYED_BY = ((1, 3, None, 1), (1, 3, 3, 1))
BATCHES = ((0, 256), (256, 512), (768, 512), (1280, 256))


def place():
    z = lax.axis_index("group")
    s = lax.axis_index("shard")
    x, y, c = s // 8, (s // 2) % 4, s % 2
    u = y * (1 - c) + x * c
    v = x * (1 - c) + y * c
    return z, u, v, c


def at(z, u, v, c):
    x = v * (1 - c) + u * c
    y = u * (1 - c) + v * c
    return (z, (x * 4 + y) * 2 + c)


def own_slot(far, c):
    return {0: 0, 1: 4 - 2 * c, 3: 5 - 2 * c, 2: 6}[far]


def other_slot(far, c):
    return {0: 1, 1: 2 + 2 * c, 3: 3 + 2 * c, 2: 7}[far]


def rows_of(slot, v):
    return pl.ds(pl.multiple_of(slot * UNIT + v * BLOCK, 16), BLOCK)


def meet(others):
    barrier = pltpu.get_barrier_semaphore()
    for other in others:
        pl.semaphore_signal(barrier, inc=1, device_id=other, device_id_type=MESH)
    pl.semaphore_wait(barrier, len(others))


def flat_place(l, colour, u):
    v = (l * 1366) >> 16
    l = l - v * BLOCK
    z = (l * 10923) >> 16
    r = l - z * PER
    chip = v * (4 - 3 * colour) + u * (1 + 3 * colour)
    return z * UNIT + chip * 2 * PER + colour * PER + r


def exact_parts(a):
    high = a.astype(BF16)
    rest = a - high.astype(F32)
    middle = rest.astype(BF16)
    return high, middle, (rest - middle.astype(F32)).astype(BF16)


def own_targets(targets, owner, rows, slots):
    local = targets - owner * rows
    local = jnp.where((local >= 0) & (local < rows), local, rows)
    pad = jnp.zeros((4, 128), jnp.int32)
    both = jnp.concatenate([local >> 6, pad, local & 63, pad], axis=0).astype(F32).astype(BF16)
    lines = []
    for colour, u in slots:
        flat = flat_place(lax.broadcasted_iota(jnp.int32, (1, UNIT), 1), colour, u)
        lane = lax.broadcasted_iota(jnp.int32, (128, UNIT), 0) == (flat & 127)
        found = jnp.dot(both, jnp.where(lane, 1.0, 0.0).astype(BF16), preferred_element_type=F32)
        row = lax.broadcasted_iota(jnp.int32, (16, UNIT), 0) == (flat >> 7)
        value = jnp.where(row, found[0:16] * 64.0 + found[16:32], 0.0)
        lines.append(jnp.sum(value, axis=0, keepdims=True))
    return jnp.concatenate(lines, axis=1).astype(jnp.int32)


def selector(colour, u, half):
    flat = flat_place(lax.broadcasted_iota(jnp.int32, (128, 128), 0) + half * 64, colour, u)
    lane = lax.broadcasted_iota(jnp.int32, (128, 128), 1) == (flat & 127)
    return jnp.where(lane, 1.0, 0.0).astype(BF16)


def in_order(loss, select, colour, u):
    total = None
    for half in range(2):
        l = lax.broadcasted_iota(jnp.int32, (16, 128), 1) + half * 64
        here = lax.broadcasted_iota(jnp.int32, (16, 128), 0) == (flat_place(l, colour, u) >> 7)
        here = here & (l >= half * 128)
        parts = [jnp.where(here, part.astype(F32), 0.0).astype(BF16) for part in exact_parts(loss[half : half + 1])]
        found = jnp.dot(jnp.concatenate(parts, axis=0), select[half], preferred_element_type=F32)
        total = found if total is None else total + found
    return (total[0:16] + total[16:32]) + total[32:48]


def scored_batch(c_buf, q_ref, t_ref, first, cols, s0, s1, between, before):
    rows = s0.shape[0]
    blocks = c_buf.shape[0] // rows
    groups = rows // 8
    q_rows = pl.ds(first, cols)
    wanted = jnp.broadcast_to(t_ref[:, first : first + cols], (8, cols))
    wanted = wanted - lax.broadcasted_iota(jnp.int32, (8, cols), 0)

    def scored(k, held):
        part = c_buf[pl.ds(pl.multiple_of(k * rows, rows), rows), :]
        scores = lax.dot_general(part, q_ref[q_rows, :], (((1,), (1,)), ((), ())), preferred_element_type=F32)
        held[...] = scores
        return scores

    def peak(scores, top):
        return jnp.maximum(top, jnp.max(scores.reshape(groups, 8, cols), axis=0))

    def take(held, k, old, new, total, picked):
        total = total * jnp.exp(old - new)
        for g in range(groups):
            value = held[g * 8 : (g + 1) * 8, :]
            total = total + jnp.exp(value - new)
            picked = jnp.where(wanted == k * rows + g * 8, value, picked)
        return total, picked

    def step(j, carry):
        old, new, total, picked = carry
        newer = peak(scored(2 * j + 1, s1), new)
        total, picked = take(s0, 2 * j, old, new, total, picked)
        newest = peak(scored(2 * j + 2, s0), newer)
        total, picked = take(s1, 2 * j + 1, new, newer, total, picked)
        return newer, newest, total, picked

    old = jnp.full((8, cols), LOW, F32)
    zero = jnp.zeros((8, cols), F32)
    carry = (old, peak(scored(0, s0), old), zero, zero)
    before()
    pairs = blocks // 2 - 1
    for k, handle in enumerate(between):
        if handle is not None:
            handle()
        if k < pairs:
            carry = lax.fori_loop(k, k + 1, step, carry)
    carry = lax.fori_loop(min(len(between), pairs), pairs, step, carry)
    old, new, total, picked = carry
    newer = peak(scored(blocks - 1, s1), new)
    total, picked = take(s0, blocks - 2, old, new, total, picked)

    def finish():
        last, found = take(s1, blocks - 1, new, newer, total, picked)
        top = jnp.max(newer, axis=0, keepdims=True)
        last = jnp.sum(last * jnp.exp(newer - top), axis=0, keepdims=True)
        return top, last, jnp.sum(found, axis=0, keepdims=True)

    return finish


def loss_kernel(
    q_hbm, c_hbm, t_hbm, o_ref, mean_ref,
    t_nat, t_ref, select, c_buf, all_ref, first, narrow0, narrow1, wide0, wide1,
    partial, from_row, at_y, from_y, at_z, from_z, shared,
    small, loaded, send1, recv1, send2, recv2, send3, recv3, sendp, recvp, sends, recvs,
):
    z, u, v, c = place()
    x = v * (1 - c) + u * c
    y = u * (1 - c) + v * c

    def device(z, x, y, c):
        return (z, (x * 4 + y) * 2 + c)

    chunk = c_buf.shape[0] // loaded.shape[0]
    loads = [
        pltpu.make_async_copy(c_hbm.at[pl.ds(i * chunk, chunk)], c_buf.at[pl.ds(i * chunk, chunk)], loaded.at[i])
        for i in range(loaded.shape[0])
    ]
    ask = pltpu.make_async_copy(q_hbm, first.at[z], small.at[0])
    ask_t = pltpu.make_async_copy(t_hbm, t_nat, small.at[1])
    ask.start()
    ask_t.start()
    partner = device(z, x, y, 1 - c)
    column = [device((z + d) % 8, x, y, c) for d in range(1, 8)]
    xs = [device(z, (x + d) % 4, y, c) for d in range(1, 4)]
    ys = [device(z, x, (y + d) % 4, c) for d in range(1, 4)]
    crossed = [device(z, (x + d) % 4, y, 1 - c) for d in range(1, 4)]
    along_v = {d: at(z, u, (v + d) % 4, c) for d in NEAR_FIRST}
    along_u = {d: at(z, (u + d) % 4, v, c) for d in NEAR_FIRST}
    meet(column + xs + ys + crossed + [partner])
    for load in loads:
        load.start()
    ask.wait()

    def copy(src, dst, send, recv, to):
        return pltpu.make_async_remote_copy(
            src_ref=src, dst_ref=dst, send_sem=send, recv_sem=recv, device_id=to, device_id_type=MESH
        )

    def start(*args):
        copy(*args).start()

    for d in (4, 3, 5, 2, 6, 1, 7):
        start(first.at[z], first.at[z], send1.at[d], recv1.at[d], column[d - 1])
    slots = [(c, u), (1 - c, v), (1, (x + 1) % 4), (1, (x + 3) % 4)]
    slots += [(0, (y + 1) % 4), (0, (y + 3) % 4), (c, (u + 2) % 4), (1 - c, (v + 2) % 4)]
    ask_t.wait()
    owner = z * 32 + lax.axis_index("shard")
    t_ref[...] = own_targets(t_nat[...], owner, c_buf.shape[0], slots)
    for half in range(2):
        select[half] = selector(c, x, half)
    for d in (1, 7, 2, 6, 3, 5, 4):
        here = first.at[(z + 8 - d) % 8]
        copy(here, here, send1.at[d], recv1.at[d], column[d - 1]).wait_recv()
    block = jnp.concatenate([first[k].astype(F32) for k in range(8)], axis=0)
    all_ref[rows_of(0, v), :] = block.astype(BF16)

    def to_partner(far, d):
        held = all_ref.at[rows_of(own_slot(far, c), (v + 4 - d) % 4)]
        there = all_ref.at[rows_of(other_slot(far, 1 - c), (v + 4 - d) % 4)]
        start(held, there, sendp.at[far, d], recvp.at[far, d], partner)

    def along(e, d):
        held = all_ref.at[rows_of(0, (v + 4 - d) % 4)]
        there = all_ref.at[rows_of(own_slot((4 - e) % 4, c), (v + 4 - d) % 4)]
        start(held, there, send3.at[e, d], recv3.at[e, d], along_u[e])

    def arrived_along(e, d):
        here = all_ref.at[rows_of(own_slot((4 - e) % 4, c), (v + 4 - d) % 4)]
        copy(here, here, send3.at[e, d], recv3.at[e, d], along_u[e]).wait_recv()

    def from_partner(far):
        for d in range(4):
            here = all_ref.at[rows_of(other_slot(far, c), (u + 4 - d) % 4)]
            copy(here, here, sendp.at[far, d], recvp.at[far, d], partner).wait_recv()

    own = all_ref.at[rows_of(0, v)]
    for d in (2, 1, 3):
        start(own, own, send2.at[d], recv2.at[d], along_v[d])
    to_partner(0, 0)
    along(1, 0)
    along(3, 0)
    for d in NEAR_FIRST:
        here = all_ref.at[rows_of(0, (v + 4 - d) % 4)]
        copy(here, here, send2.at[d], recv2.at[d], along_v[d]).wait_recv()
        to_partner(0, d)
        along(1, d)
        along(3, d)
    pl.when(c == 0)(lambda: along(2, 2))

    def near_blocks(core, *ds):
        for d in ds:
            for e in (1, 3):
                arrived_along(e, d)
                if e == RELAYED_BY[core][d]:
                    held = all_ref.at[rows_of(own_slot((4 - e) % 4, c), (v + 4 - d) % 4)]
                    there = all_ref.at[rows_of(own_slot(2, c), (v + 4 - d) % 4)]
                    start(held, there, send3.at[2, d], recv3.at[2, d], along_u[e])
                to_partner((4 - e) % 4, d)

    def on_core(core, handle, *ds):
        pl.when(c == core)(lambda: handle(core, *ds))

    def near_from_partner(core):
        from_partner(1)
        from_partner(3)

    on_core(1, near_blocks, 0, 1, 3, 2)
    on_core(0, near_blocks, 0)
    for load in loads:
        load.wait()
    from_partner(0)

    results = []
    ends = []

    def end():
        if ends:
            results.append(ends.pop()())

    def run(k, between=()):
        begin, cols = BATCHES[k]
        held = (narrow0, narrow1) if cols == narrow0.shape[1] else (wide0, wide1)
        ends.append(scored_batch(c_buf, all_ref, t_ref, begin, cols, *held, between, end))

    run(0)
    on_core(0, near_blocks, 1)
    on_core(0, near_from_partner)
    run(1, (None, lambda: on_core(0, near_blocks, 3), lambda: on_core(0, near_blocks, 2)))
    for d in (0, 1, 3, 2):
        arrived_along(2, d)
        to_partner(2, d)
    on_core(1, near_from_partner)
    run(2, (None, None, None))
    from_partner(2)
    run(3)
    end()

    lines = [jnp.concatenate(parts, axis=1) for parts in zip(*results)]
    for slot, (colour, there) in enumerate(slots):
        parts = []
        for line in lines:
            parts.append(line[:, slot * UNIT : slot * UNIT + 128])
            parts.append(line[:, slot * UNIT + 64 : slot * UNIT + 192])
        partial[colour * 4 + there] = jnp.concatenate(parts + [jnp.zeros((2, 128), F32)], axis=0)

    def pass_on(k, src, dst, to):
        start(src, dst, sends.at[k], recvs.at[k], to)

    def wait(k, here):
        copy(here, here, sends.at[k], recvs.at[k], partner).wait_recv()

    unit = c * 4 + x
    row = [None] + [((x + k // 2) % 4, (c + k) % 2) for k in range(1, 8)]
    for k in (4, 5, 2, 3, 6, 7, 1):
        there, core = row[k]
        pass_on(13 + k, partial.at[core * 4 + there], from_row.at[k], device(z, there, y, core))
    for k in range(1, 8):
        wait(13 + k, from_row.at[k])
    at_y[...] = combined([partial[unit]] + [from_row[k] for k in range(1, 8)])
    for d in range(1, 4):
        pass_on(3 + d, at_y, from_y.at[d], ys[d - 1])
    for d in range(1, 4):
        wait(3 + d, from_y.at[d])
    at_z[...] = combined([at_y[...]] + [from_y[d] for d in range(1, 4)])
    for d in (4, 3, 5, 2, 6, 1, 7):
        pass_on(6 + d, at_z, from_z.at[d], column[d - 1])
    for d in range(1, 8):
        wait(6 + d, from_z.at[d])
    whole = combined([at_z[...]] + [from_z[d] for d in range(1, 8)])
    loss = whole[0:2] + jnp.log(whole[2:4]) - whole[4:6]
    shared[0] = in_order(loss, select, c, x)
    for k in (4, 5, 2, 3, 6, 7, 1):
        there, core = row[k]
        pass_on(20 + k, shared.at[0], shared.at[k], device(z, there, y, core))
    for k in range(1, 8):
        wait(20 + k, shared.at[k])
    every = ((shared[0] + shared[1]) + (shared[2] + shared[3])) + ((shared[4] + shared[5]) + (shared[6] + shared[7]))
    o_ref[...] = every[0:12]
    mean_ref[...] = jnp.sum(every, keepdims=True) * (1.0 / (8 * UNIT))
    for d in range(1, 8):
        copy(first.at[z], first.at[z], send1.at[d], recv1.at[d], partner).wait_send()
    for d in range(4):
        if d:
            copy(own, own, send2.at[d], recv2.at[d], partner).wait_send()
        for e in range(4):
            copy(own, own, sendp.at[e, d], recvp.at[e, d], partner).wait_send()
            if e:
                copy(own, own, send3.at[e, d], recv3.at[e, d], partner).wait_send()
    for k in range(1, 8):
        if k < 4:
            copy(at_y, at_y, sends.at[3 + k], recvs.at[3 + k], partner).wait_send()
        copy(at_z, at_z, sends.at[6 + k], recvs.at[6 + k], partner).wait_send()
        copy(at_z, at_z, sends.at[13 + k], recvs.at[13 + k], partner).wait_send()
        copy(shared.at[0], shared.at[0], sends.at[20 + k], recvs.at[20 + k], partner).wait_send()


def all_losses(queries, candidates, targets):
    count, width = candidates.shape
    tile = (8, 128)
    dma = pltpu.SemaphoreType.DMA
    return pl.pallas_call(
        loss_kernel,
        out_shape=(jax.ShapeDtypeStruct((12, 128), F32), jax.ShapeDtypeStruct((1, 1), F32)),
        in_specs=[
            pl.BlockSpec(memory_space=pltpu.HBM),
            pl.BlockSpec(memory_space=pltpu.HBM),
            pl.BlockSpec(memory_space=pltpu.HBM),
        ],
        out_specs=(pl.BlockSpec(memory_space=pltpu.VMEM), pl.BlockSpec(memory_space=pltpu.VMEM)),
        scratch_shapes=[
            pltpu.VMEM((12, 128), jnp.int32),
            pltpu.VMEM((1, 8 * UNIT), jnp.int32),
            pltpu.VMEM((2, 128, 128), BF16),
            pltpu.VMEM((count, width), BF16),
            pltpu.VMEM((8 * UNIT, width), BF16),
            pltpu.VMEM((8, PER, width), BF16),
            pltpu.VMEM((1024, 256), F32),
            pltpu.VMEM((1024, 256), F32),
            pltpu.VMEM((512, 512), F32),
            pltpu.VMEM((512, 512), F32),
            pltpu.VMEM((8, *tile), F32),
            pltpu.VMEM((8, *tile), F32),
            pltpu.VMEM(tile, F32),
            pltpu.VMEM((4, *tile), F32),
            pltpu.VMEM(tile, F32),
            pltpu.VMEM((8, *tile), F32),
            pltpu.VMEM((8, 16, 128), F32),
        ]
        + [dma((2,)), dma((4,)), dma((8,)), dma((8,)), dma((4,)), dma((4,)), dma((4, 4)), dma((4, 4)), dma((4, 4)), dma((4, 4))]
        + [dma((28,)), dma((28,))],
        compiler_params=pltpu.CompilerParams(
            collective_id=1, has_side_effects=True, vmem_limit_bytes=50 << 20
        ),
        name="ranking_losses",
    )(queries, candidates, targets)


def combined(tiles):
    tops = [tile[0:2] for tile in tiles]
    top = functools.reduce(jnp.maximum, tops)
    total = sum(tile[2:4] * jnp.exp(one - top) for tile, one in zip(tiles, tops))
    picked = sum(tile[4:6] for tile in tiles)
    return jnp.concatenate([top, total, picked, jnp.zeros((2, 128), F32)], axis=0)


def on_device(queries, candidates, targets):
    held = (queries, candidates, targets.reshape(12, 128))
    losses, mean = all_losses(*(pltpu.with_memory_space_constraint(a, pltpu.HBM) for a in held))
    return losses.reshape(-1), mean[0, 0]


def solution(mesh):
    whole = P(("group", "shard"), None)
    return jax.shard_map(
        on_device, mesh=mesh, in_specs=(whole, whole, P()), out_specs=(P(), P()), check_vma=False
    )
```
